512 devices in a mesh: sx: 16 (over z, x_hi), sy: 32 (over y, x_lo, core).
Axes of the slice: x: 4 (x_hi: 2, x_lo: 2; x = x_hi * 2 + x_lo), y: 8, z: 8, core: 2. Of those that a mesh axis runs over, the one named last changes fastest.
Arguments:
- coeffs: float32 [2, 32, 32, 16, 256], P(None, 'sx', 'sy'), may hold values from -6 to 6
- source_nodes: float32 [3, 2, 32, 32, 256], P(None, None, 'sx', 'sy'), may hold values from 0.2 to 1
- target_nodes: float32 [3, 2, 2, 2, 32, 32, 256], P(None, None, None, None, 'sx', 'sy'), may hold values from 0.2 to 1
- interp_rows: float32 [3, 2, 16, 16], replicated, may hold values from -1 to 1
- interp_cols: float32 [3, 2, 16, 16], replicated, may hold values from -1 to 1
Outputs:
- field: float32 [2, 32, 32, 16, 256], P(None, 'sx', 'sy')
The draws below stay inside these ranges and needn't reach their ends.
All inputs are finite; a program needn't handle non-finite values.
Results may differ from the reference program's by a relative error of at most 0.0003.
Values sent between devices are 32-bit elements; how exact they have to be, the bound alone decides.
No kernel may reach another device: no remote copies, remote signals or barrier semaphores. Data moves between devices by JAX's collectives and lax.ppermute only.
A program may use at most 64 MiB of HBM per device.

```python
import jax
import jax.numpy as jnp
from jax import lax

CHEB = 16
NODES = 256
RHS = 16
BOX_ROWS = 2
BOX_COLS = 1
LEVELS = 3
NBR = 32
NBC = 32
N_SX = 16
N_SY = 32


def block_scale(key, shape, split, least, high):
    gain, own = 1.0, jax.random.fold_in(key, 6)
    for position, blocks in split:
        draws = jnp.exp(jax.random.uniform(jax.random.fold_in(own, position), (blocks,), jnp.float32, least / len(split), high / len(split)))
        gain = gain * jnp.repeat(draws, shape[position] // blocks).reshape([-1 if axis == position else 1 for axis in range(len(shape))])
    return gain


def bell_draw(rng, dims, spread, limit, pieces=(), kind=jnp.bfloat16):
    entries = spread * jax.random.normal(rng, dims, jnp.float32)
    if pieces:
        entries = entries * block_scale(rng, dims, pieces, -0.22, 0.18)
    return jnp.clip(entries, -limit, limit).astype(kind)


def setup_inputs(seed: int = 0) -> dict:
    keys = jax.random.split(jax.random.key(seed), 6)
    coeffs = bell_draw(keys[0], (2, NBR, NBC, RHS, NODES), 1.0, 6.0, ((1, 16), (2, 32)), jnp.float32)
    source_nodes = jnp.clip(0.2 + 0.8 * jax.random.uniform(keys[1], (LEVELS, 2, NBR, NBC, NODES), jnp.float32) ** block_scale(keys[1], (LEVELS, 2, NBR, NBC, NODES), ((2, 16), (3, 32)), -0.2, 0.2), 0.2, 1.0)
    target_nodes = jnp.clip(0.2 + 0.8 * jax.random.uniform(keys[2], (LEVELS, 2, 2, 2, NBR, NBC, NODES), jnp.float32) ** block_scale(keys[2], (LEVELS, 2, 2, 2, NBR, NBC, NODES), ((4, 16), (5, 32)), -0.2, 0.2), 0.2, 1.0)
    interp_rows = bell_draw(keys[3], (LEVELS, 2, CHEB, CHEB), (2 * CHEB) ** -0.5, 1.0, (), jnp.float32)
    interp_cols = bell_draw(keys[4], (LEVELS, 2, CHEB, CHEB), (2 * CHEB) ** -0.5, 1.0, (), jnp.float32)
    return dict(coeffs=coeffs, source_nodes=source_nodes, target_nodes=target_nodes, interp_rows=interp_rows, interp_cols=interp_cols)


angular_scale = 25.132741228718345

def kron_of(rows_matrix, cols_matrix):
    width = rows_matrix.shape[0]
    return (rows_matrix[:, None, :, None] * cols_matrix[None, :, None, :]).reshape(width * width, width * width)

def translate_one(values, source, target, kron_matrix):
    angles = angular_scale * source[0][None, :] * jnp.sqrt(target[0][:, None] * target[0][:, None] + target[1][:, None] * source[1][None, :] * (target[1][:, None] * source[1][None, :]))
    weights = jnp.concatenate([kron_matrix * jnp.cos(angles), kron_matrix * jnp.sin(angles)], axis=0)
    gathers = values.shape[1]
    points = values.shape[2]
    stacked = values.reshape(2 * gathers, points)
    product = jnp.einsum('rs,ts->rt', stacked, weights, precision=lax.Precision.HIGHEST)
    real_out = product[:gathers, :points] - product[gathers:, points:]
    imag_out = product[:gathers, points:] + product[gathers:, :points]
    return jnp.stack([real_out, imag_out])

def translate_boxes(current, source, target, kron_matrix):
    rows_count, cols_count = (current.shape[1], current.shape[2])
    gathers, points = (current.shape[3], current.shape[4])
    values = current.transpose(1, 2, 0, 3, 4).reshape(rows_count * cols_count, 2, gathers, points)
    sources = source.transpose(1, 2, 0, 3).reshape(rows_count * cols_count, 2, points)
    targets = target.transpose(1, 2, 0, 3).reshape(rows_count * cols_count, 2, points)
    result = lax.map(lambda item: translate_one(item[0], item[1], item[2], kron_matrix), (values, sources, targets))
    return result.reshape(rows_count, cols_count, 2, gathers, points).transpose(2, 0, 1, 3, 4)

def reference(coeffs, source_nodes, target_nodes, interp_rows, interp_cols):
    rows_log = N_SX.bit_length() - 1
    cols_log = N_SY.bit_length() - 1
    row_ids = jnp.arange(NBR, dtype=jnp.int32)
    col_ids = jnp.arange(NBC, dtype=jnp.int32)
    current = coeffs
    for level_index in range(LEVELS):
        bit_rows = level_index % rows_log
        bit_cols = level_index % cols_log
        row_bits = row_ids // BOX_ROWS // 2 ** bit_rows % 2
        col_bits = col_ids // BOX_COLS // 2 ** bit_cols % 2
        total = jnp.zeros_like(current)
        for row_pos in range(2):
            for col_pos in range(2):
                kron_matrix = kron_of(interp_rows[level_index, row_pos], interp_cols[level_index, col_pos])
                translated = translate_boxes(current, source_nodes[level_index], target_nodes[level_index, :, row_pos, col_pos], kron_matrix)
                mask = (row_bits[:, None] == row_pos) & (col_bits[None, :] == col_pos)
                summed = jnp.zeros_like(current)
                for row_move in range(2):
                    partner_rows = (row_ids + row_move * BOX_ROWS * 2 ** bit_rows * (1 - 2 * row_bits)).astype(jnp.int32)
                    for col_move in range(2):
                        partner_cols = (col_ids + col_move * BOX_COLS * 2 ** bit_cols * (1 - 2 * col_bits)).astype(jnp.int32)
                        summed = summed + translated[:, partner_rows][:, :, partner_cols]
                total = total + jnp.where(mask[None, :, :, None, None], summed, jnp.zeros_like(summed))
        current = total
    return current
```

```python
import functools
import math

import jax
import jax.numpy as jnp
import numpy as np
from jax import lax
from jax.experimental import pallas as pl
from jax.experimental.pallas import tpu as pltpu
from jax.sharding import PartitionSpec as P

LEVELS = 3
CHEB = 16
NODES = CHEB * CHEB
RHS = 16
BOXES = 2
KERNELS = 4 * BOXES
ROOT2 = math.sqrt(2.0)


def half_turn_coefficients():
    nodes = 0.5 * np.cos((np.arange(64) + 0.5) * np.pi / 128)
    powers = np.stack([nodes, nodes**3, nodes**5], axis=1)
    wanted = 2.0**0.75 * np.sin(0.5 * np.pi * nodes)
    return [float(c) for c in np.linalg.lstsq(powers, wanted, rcond=None)[0]]


C0, C1, C2 = half_turn_coefficients()


def group_members(mesh, bit):
    n_rows, n_cols = mesh.shape["sx"], mesh.shape["sy"]
    step = 1 << bit
    groups = []
    for row in range(n_rows):
        for col in range(n_cols):
            if not row & step and not col & step:
                groups.append(
                    [(row + a) * n_cols + col + c for a in (0, step) for c in (0, step)]
                )
    return groups


def prepare(level, sources, rows, cols, a_ref, b_ref, row_ref, col_ref):
    lane = lax.broadcasted_iota(jnp.int32, (CHEB, NODES), 1)
    node = lax.broadcasted_iota(jnp.int32, (CHEB, NODES), 0)
    outer = (lane // CHEB == node).astype(jnp.float32)
    inner = (lane % CHEB == node).astype(jnp.float32)
    spread = functools.partial(
        lax.dot_general,
        dimension_numbers=(((0,), (0,)), ((), ())),
        precision=lax.Precision.HIGHEST,
        preferred_element_type=jnp.float32,
    )
    for bit in range(2):
        row_ref[bit] = spread(rows[level, bit], outer)
        col_ref[bit] = spread(cols[level, bit], inner)
    lines = []
    for box in range(BOXES):
        freq = sources[level, 0, box]
        slow = sources[level, 1, box]
        near = 16.0 * freq * freq
        lines += [near, near * slow * slow]
    columns = jnp.concatenate(lines + lines, axis=0).T
    for box in range(BOXES):
        a_ref[box] = jnp.broadcast_to(columns[:, 2 * box : 2 * box + 1], (NODES, 128))
        b_ref[box] = jnp.broadcast_to(columns[:, 2 * box + 1 : 2 * box + 2], (NODES, 128))


def weigh(level, targets, a_ref, b_ref, row_ref, col_ref, high, low):
    for box in range(BOXES):
        squares = []
        for pos in range(4):
            tau = targets[level, 0, pos // 2, pos % 2, box]
            off = targets[level, 1, pos // 2, pos % 2, box]
            squares.append((tau * tau, off * off))

        def strip(step, carry):
            down = pl.ds(step * CHEB, CHEB)
            along = pl.ds(NODES + step * CHEB, CHEB)
            near = a_ref[box, down, :]
            far = b_ref[box, down, :]
            near = jnp.concatenate([near, near], axis=1)
            far = jnp.concatenate([far, far], axis=1)
            for pos in range(4):
                tau2, off2 = squares[pos]
                kron = row_ref[pos // 2, pl.ds(step, 1), :] * col_ref[pos % 2]
                z = near * tau2 + far * off2
                turns = z * lax.rsqrt(z)
                rest = turns - jnp.round(turns)
                y = rest * rest
                half = rest * (C0 + y * (C1 + y * C2))
                q = half * half
                cosine = ROOT2 - q
                v = 2.0 * ROOT2 - q
                sine = half * (v * lax.rsqrt(v))
                part = kron * sine
                real = kron - part * sine
                imag = part * cosine
                item = box * 4 + pos
                for where, value in ((down, real), (along, imag)):
                    top = value.astype(jnp.bfloat16)
                    high[item, where, :] = top
                    low[item, where, :] = (value - top.astype(jnp.float32)).astype(jnp.bfloat16)
            return carry

        lax.fori_loop(0, CHEB, strip, 0)


def apply(box, values, high, low, out):
    def turned(x):
        return jnp.concatenate([-x[RHS:], x[:RHS]], axis=0)

    top = values.astype(jnp.bfloat16)
    rest = (values - top.astype(jnp.float32)).astype(jnp.bfloat16)
    left = jnp.concatenate([top, rest], axis=0)
    right = jnp.concatenate([turned(top), turned(rest)], axis=0)
    both = jnp.concatenate([left, right], axis=1)
    for pos in range(4):
        item = box * 4 + pos
        main = jnp.dot(both, high[item], preferred_element_type=jnp.float32)
        small = jnp.dot(both[: 2 * RHS], low[item], preferred_element_type=jnp.float32)
        total = main[: 2 * RHS] + main[2 * RHS :] + small
        out[pos, pl.ds(box * RHS, RHS), :] = total[:RHS]
        out[pos, pl.ds((BOXES + box) * RHS, RHS), :] = total[RHS:]


def first_kernel(coeffs, sources, targets, rows, cols, out, a_ref, b_ref, row_ref, col_ref, high, low):
    prepare(0, sources, rows, cols, a_ref, b_ref, row_ref, col_ref)
    weigh(0, targets, a_ref, b_ref, row_ref, col_ref, high, low)
    for box in range(BOXES):
        values = jnp.concatenate([coeffs[0, box], coeffs[1, box]], axis=0)
        apply(box, values, high, low, out)


def weights_kernel(level, sources, targets, rows, cols, high, low, a_ref, b_ref, row_ref, col_ref):
    prepare(level, sources, rows, cols, a_ref, b_ref, row_ref, col_ref)
    weigh(level, targets, a_ref, b_ref, row_ref, col_ref, high, low)


def later_kernel(pieces, high, low, out):
    summed = (pieces[0] + pieces[1]) + (pieces[2] + pieces[3])
    for box in range(BOXES):
        values = jnp.concatenate(
            [
                summed[box * RHS : (box + 1) * RHS],
                summed[(BOXES + box) * RHS : (BOXES + box + 1) * RHS],
            ],
            axis=0,
        )
        apply(box, values, high, low, out)


TABLES = (
    pltpu.VMEM((BOXES, NODES, 128), jnp.float32),
    pltpu.VMEM((BOXES, NODES, 128), jnp.float32),
    pltpu.VMEM((2, CHEB, NODES), jnp.float32),
    pltpu.VMEM((2, CHEB, NODES), jnp.float32),
)
WEIGHTS = pltpu.VMEM((KERNELS, 2 * NODES, NODES), jnp.bfloat16)
SENT = pltpu.VMEM((4, 2 * BOXES * RHS, NODES), jnp.float32)
SMALL = pltpu.CompilerParams(vmem_limit_bytes=12 * 1024 * 1024)


def solution(mesh):
    groups = [group_members(mesh, bit) for bit in range(LEVELS)]

    def exchange(sent, level):
        return lax.all_to_all(
            sent, ("sx", "sy"), 0, 0, axis_index_groups=groups[level], tiled=True
        )

    def local(coeffs, source_nodes, target_nodes, interp_rows, interp_cols):
        coeffs = coeffs.reshape(2, BOXES, RHS, NODES)
        sources = source_nodes.reshape(LEVELS, 2, BOXES, 1, NODES)
        targets = target_nodes.reshape(LEVELS, 2, 2, 2, BOXES, 1, NODES)
        sent = pl.pallas_call(
            first_kernel,
            out_shape=SENT,
            scratch_shapes=TABLES + (WEIGHTS, WEIGHTS),
            compiler_params=SMALL,
            name="first",
        )(coeffs, sources, targets, interp_rows, interp_cols)
        made = [
            pl.pallas_call(
                functools.partial(weights_kernel, level),
                out_shape=(WEIGHTS, WEIGHTS),
                scratch_shapes=TABLES,
                compiler_params=SMALL,
                cost_estimate=pl.CostEstimate(
                    flops=60_000_000, bytes_accessed=100_000, transcendentals=0
                ),
                name=f"weights_{level}",
            )(sources, targets, interp_rows, interp_cols)
            for level in range(1, LEVELS)
        ]
        for level in range(1, LEVELS):
            sent = pl.pallas_call(
                later_kernel, out_shape=SENT, compiler_params=SMALL, name=f"later_{level}"
            )(exchange(sent, level - 1), *made[level - 1])
        pieces = exchange(sent, LEVELS - 1)
        field = (pieces[0] + pieces[1]) + (pieces[2] + pieces[3])
        return field.reshape(2, BOXES, 1, RHS, NODES)

    in_specs = (
        P(None, "sx", "sy", None, None),
        P(None, None, "sx", "sy", None),
        P(None, None, None, None, "sx", "sy", None),
        P(),
        P(),
    )
    out_specs = P(None, "sx", "sy", None, None)
    return jax.shard_map(local, mesh=mesh, in_specs=in_specs, out_specs=out_specs, check_vma=False)
```

```python
import functools
import math

import jax
import jax.numpy as jnp
import numpy as np
from jax import lax
from jax.experimental import pallas as pl
from jax.experimental.pallas import tpu as pltpu
from jax.sharding import PartitionSpec as P

LEVELS = 3
CHEB = 16
NODES = CHEB * CHEB
RHS = 16
BOXES = 2
FOREIGN = 3
ITEMS = FOREIGN * BOXES
ROOT2 = math.sqrt(2.0)


def half_turn_coefficients():
    nodes = 0.5 * np.cos((np.arange(64) + 0.5) * np.pi / 128)
    powers = np.stack([nodes, nodes**3, nodes**5], axis=1)
    wanted = 2.0**0.75 * np.sin(0.5 * np.pi * nodes)
    return [float(c) for c in np.linalg.lstsq(powers, wanted, rcond=None)[0]]


C0, C1, C2 = half_turn_coefficients()


def group_members(mesh, bit):
    n_rows, n_cols = mesh.shape["sx"], mesh.shape["sy"]
    step = 1 << bit
    groups = []
    for row in range(n_rows):
        for col in range(n_cols):
            if not row & step and not col & step:
                groups.append(
                    [(row + a) * n_cols + col + c for a in (0, step) for c in (0, step)]
                )
    return groups


def fetch(pairs, sems):
    copies = [pltpu.make_async_copy(a, b, sems.at[i]) for i, (a, b) in enumerate(pairs)]
    for copy in copies:
        copy.start()
    return copies


def own_position(level):
    step = 1 << level
    row = lax.axis_index("sx") // step % 2
    col = lax.axis_index("sy") // step % 2
    return 2 * row + col


def prepare(sources, rows, cols, tables):
    a_ref, b_ref, row_ref, col_ref = tables
    lane = lax.broadcasted_iota(jnp.int32, (CHEB, NODES), 1)
    node = lax.broadcasted_iota(jnp.int32, (CHEB, NODES), 0)
    outer = (lane // CHEB == node).astype(jnp.float32)
    inner = (lane % CHEB == node).astype(jnp.float32)
    spread = functools.partial(
        lax.dot_general,
        dimension_numbers=(((0,), (0,)), ((), ())),
        precision=lax.Precision.HIGHEST,
        preferred_element_type=jnp.float32,
    )
    for bit in range(2):
        row_ref[bit] = spread(rows[bit], outer)
        col_ref[bit] = spread(cols[bit], inner)
    lines = []
    for box in range(BOXES):
        freq = sources[0, box]
        slow = sources[1, box]
        near = 16.0 * freq * freq
        lines += [near, near * slow * slow]
    columns = jnp.concatenate(lines + lines, axis=0).T
    for box in range(BOXES):
        a_ref[box] = jnp.broadcast_to(columns[:, 2 * box : 2 * box + 1], (NODES, 128))
        b_ref[box] = jnp.broadcast_to(columns[:, 2 * box + 1 : 2 * box + 2], (NODES, 128))


def weigh(position, box, targets, tables, high, low):
    a_ref, b_ref, row_ref, col_ref = tables
    row_bit, col_bit = position // 2, position % 2
    tau = targets[0, row_bit, col_bit, box]
    off = targets[1, row_bit, col_bit, box]
    tau2, off2 = tau * tau, off * off
    inner = col_ref[col_bit]
    for step in range(CHEB):
        down = pl.ds(step * CHEB, CHEB)
        along = pl.ds(NODES + step * CHEB, CHEB)
        near = a_ref[box, down, :]
        far = b_ref[box, down, :]
        near = jnp.concatenate([near, near], axis=1)
        far = jnp.concatenate([far, far], axis=1)
        kron = row_ref[row_bit, pl.ds(step, 1), :] * inner
        z = near * tau2 + far * off2
        turns = z * lax.rsqrt(z)
        rest = turns - jnp.round(turns)
        y = rest * rest
        half = rest * (C0 + y * (C1 + y * C2))
        q = half * half
        cosine = ROOT2 - q
        v = 2.0 * ROOT2 - q
        sine = half * (v * lax.rsqrt(v))
        part = kron * sine
        real = kron - part * sine
        imag = part * cosine
        for where, value in ((down, real), (along, imag)):
            top = value.astype(jnp.bfloat16)
            high[where, :] = top
            low[where, :] = (value - top.astype(jnp.float32)).astype(jnp.bfloat16)


def stacked(values):
    def turned(x):
        return jnp.concatenate([-x[RHS:], x[:RHS]], axis=0)

    top = values.astype(jnp.bfloat16)
    rest = (values - top.astype(jnp.float32)).astype(jnp.bfloat16)
    left = jnp.concatenate([top, rest], axis=0)
    right = jnp.concatenate([turned(top), turned(rest)], axis=0)
    return jnp.concatenate([left, right], axis=1)


def stack_boxes(real, imag, left):
    for box in range(BOXES):
        left[box] = stacked(jnp.concatenate([real[box], imag[box]], axis=0))


def product(left, high, low):
    main = jnp.dot(left, high, preferred_element_type=jnp.float32)
    small = jnp.dot(left[: 2 * RHS], low, preferred_element_type=jnp.float32)
    return main[: 2 * RHS] + main[2 * RHS :] + small


def put(out, index, box, total):
    out[index, 0, box] = total[:RHS]
    out[index, 1, box] = total[RHS:]


def first_kernel(
    coeffs_hbm, sources_hbm, targets_hbm, rows_hbm, cols_hbm, out_hbm,
    coeffs, sources, targets, rows, cols, *rest,
):
    *tables, high, low, left, stage, in_sems, out_sems = rest
    nodes = fetch(
        [
            (sources_hbm.at[0], sources),
            (rows_hbm.at[0], rows),
            (cols_hbm.at[0], cols),
            (targets_hbm.at[0], targets),
            (coeffs_hbm, coeffs),
        ],
        in_sems,
    )
    me = own_position(0)
    for copy in nodes[:3]:
        copy.wait()
    prepare(sources, rows, cols, tables)
    for copy in nodes[3:]:
        copy.wait()
    stack_boxes(coeffs[0], coeffs[1], left)

    def make(item):
        slot = item % 2
        weigh(me ^ (item // 2 + 1), item % 2, targets, tables, high.at[slot], low.at[slot])

    def use(item):
        slot = item % 2
        put(stage, item // 2, item % 2, product(left[item % 2], high[slot], low[slot]))

    make(0)

    def both(item, carry):
        use(item - 1)
        make(item)
        return carry

    lax.fori_loop(1, ITEMS, both, 0)
    use(ITEMS - 1)
    sent = fetch([(stage.at[x], out_hbm.at[me ^ (x + 1)]) for x in range(FOREIGN)], out_sems)
    for copy in sent:
        copy.wait()


def between_kernel(
    level, values, sources_hbm, targets_hbm, rows_hbm, cols_hbm, own, high, low,
    sources, targets, rows, cols, *rest,
):
    *tables, own_high, own_low, left, sems = rest
    last = level == LEVELS
    count = 1 if last else 2
    here = pl.ds(level - 1, count)
    nodes = fetch(
        [
            (sources_hbm.at[here], sources),
            (rows_hbm.at[here], rows),
            (cols_hbm.at[here], cols),
            (targets_hbm.at[here], targets),
        ],
        sems,
    )
    stack_boxes(values[0], values[1], left)
    for copy in nodes:
        copy.wait()
    prepare(sources.at[0], rows.at[0], cols.at[0], tables)
    me = own_position(level - 1)

    def mine(box, carry):
        weigh(me, box, targets.at[0], tables, own_high, own_low)
        total = product(left[box], own_high[...], own_low[...])
        own[0, box] = total[:RHS]
        own[1, box] = total[RHS:]
        return carry

    lax.fori_loop(0, BOXES, mine, 0)
    if last:
        return
    prepare(sources.at[1], rows.at[1], cols.at[1], tables)
    there = own_position(level)

    def make(item, carry):
        weigh(
            there ^ (item // 2 + 1), item % 2, targets.at[1], tables, high.at[item], low.at[item]
        )
        return carry

    lax.fori_loop(0, ITEMS, make, 0)


def last_between_kernel(values, sources, targets, rows, cols, own, *rest):
    between_kernel(LEVELS, values, sources, targets, rows, cols, own, None, None, *rest)


def summed(level, pieces, own):
    me = own_position(level)
    return (own[...] + pieces[me ^ 1]) + (pieces[me ^ 2] + pieces[me ^ 3])


def later_kernel(level, pieces, own, high, low, out_hbm, current, left, stage, sems):
    values = summed(level - 1, pieces, own)
    current[...] = values
    stack_boxes(values[0], values[1], left)
    me = own_position(level)
    sent = []
    for x in range(FOREIGN):
        for box in range(BOXES):
            item = 2 * x + box
            put(stage, x, box, product(left[box], high[item], low[item]))
        copy = pltpu.make_async_copy(stage.at[x], out_hbm.at[me ^ (x + 1)], sems.at[x])
        copy.start()
        sent.append(copy)
    for copy in sent:
        copy.wait()


def final_kernel(pieces, own, out):
    out[...] = summed(LEVELS - 1, pieces, own)


def node_buffers(count):
    lead = () if count is None else (count,)
    return (
        pltpu.VMEM(lead + (2, BOXES, 1, NODES), jnp.float32),
        pltpu.VMEM(lead + (2, 2, 2, BOXES, 1, NODES), jnp.float32),
        pltpu.VMEM(lead + (2, CHEB, CHEB), jnp.float32),
        pltpu.VMEM(lead + (2, CHEB, CHEB), jnp.float32),
    )


TABLES = (
    pltpu.VMEM((BOXES, NODES, 128), jnp.float32),
    pltpu.VMEM((BOXES, NODES, 128), jnp.float32),
    pltpu.VMEM((2, CHEB, NODES), jnp.float32),
    pltpu.VMEM((2, CHEB, NODES), jnp.float32),
)
FIELD = (2, BOXES, RHS, NODES)
LEFT = pltpu.VMEM((BOXES, 4 * RHS, 2 * NODES), jnp.bfloat16)
STAGE = pltpu.VMEM((FOREIGN,) + FIELD, jnp.float32)
ANY = pl.BlockSpec(memory_space=pl.ANY)
WHOLE = pl.BlockSpec(memory_space=pltpu.VMEM)
PARAMS = pltpu.CompilerParams(vmem_limit_bytes=12 * 1024 * 1024)


def shape(dims, kind=jnp.float32):
    return jax.ShapeDtypeStruct(dims, kind)


def weights(count):
    return shape((count, 2 * NODES, NODES), jnp.bfloat16)


def cost(flops):
    return pl.CostEstimate(flops=flops, bytes_accessed=100_000, transcendentals=0)


def solution(mesh):
    groups = [group_members(mesh, bit) for bit in range(LEVELS)]

    def exchange(sent, level):
        return lax.all_to_all(
            sent, ("sx", "sy"), 0, 0, axis_index_groups=groups[level], tiled=True
        )

    def local(coeffs, source_nodes, target_nodes, interp_rows, interp_cols):
        current = coeffs.reshape(FIELD)
        nodes = (
            source_nodes.reshape(LEVELS, 2, BOXES, 1, NODES),
            target_nodes.reshape(LEVELS, 2, 2, 2, BOXES, 1, NODES),
            interp_rows,
            interp_cols,
        )
        sent = pl.pallas_call(
            first_kernel,
            in_specs=[ANY] * 5,
            out_specs=ANY,
            out_shape=shape((4,) + FIELD),
            scratch_shapes=(pltpu.VMEM(FIELD, jnp.float32),)
            + node_buffers(None)
            + TABLES
            + (pltpu.VMEM((2, 2 * NODES, NODES), jnp.bfloat16),) * 2
            + (LEFT, STAGE, pltpu.SemaphoreType.DMA((5,)), pltpu.SemaphoreType.DMA((FOREIGN,))),
            compiler_params=PARAMS,
            name="first",
        )(current, *nodes)
        for level in range(1, LEVELS + 1):
            last = level == LEVELS
            made = pl.pallas_call(
                last_between_kernel if last else functools.partial(between_kernel, level),
                in_specs=[WHOLE] + [ANY] * 4,
                out_specs=[WHOLE] * (1 if last else 3),
                out_shape=[shape(FIELD)] + ([] if last else [weights(ITEMS)] * 2),
                scratch_shapes=node_buffers(1 if last else 2)
                + TABLES
                + (pltpu.VMEM((2 * NODES, NODES), jnp.bfloat16),) * 2
                + (LEFT, pltpu.SemaphoreType.DMA((4,))),
                compiler_params=PARAMS,
                cost_estimate=cost(60_000_000),
                name=f"between_{level}",
            )(current, *nodes)
            pieces = exchange(sent, level - 1)
            if last:
                break
            sent, current = pl.pallas_call(
                functools.partial(later_kernel, level),
                in_specs=[WHOLE] * 4,
                out_specs=[ANY, WHOLE],
                out_shape=[shape((4,) + FIELD), shape(FIELD)],
                scratch_shapes=(LEFT, STAGE, pltpu.SemaphoreType.DMA((FOREIGN,))),
                compiler_params=PARAMS,
                name=f"later_{level}",
            )(pieces, *made)
        field = pl.pallas_call(
            final_kernel,
            in_specs=[WHOLE] * 2,
            out_specs=WHOLE,
            out_shape=shape(FIELD),
            compiler_params=PARAMS,
            name="final",
        )(pieces, *made)
        return field.reshape(2, BOXES, 1, RHS, NODES)

    in_specs = (
        P(None, "sx", "sy", None, None),
        P(None, None, "sx", "sy", None),
        P(None, None, None, None, "sx", "sy", None),
        P(),
        P(),
    )
    out_specs = P(None, "sx", "sy", None, None)
    return jax.shard_map(local, mesh=mesh, in_specs=in_specs, out_specs=out_specs, check_vma=False)
```

```python
import functools
import math

import jax
import jax.numpy as jnp
import numpy as np
from jax import lax
from jax.experimental import pallas as pl
from jax.experimental.pallas import tpu as pltpu
from jax.sharding import PartitionSpec as P

LEVELS = 3
CHEB = 16
NODES = CHEB * CHEB
RHS = 16
BOXES = 2
FOREIGN = 3
ITEMS = FOREIGN * BOXES
ROOT2 = math.sqrt(2.0)


def half_turn_coefficients():
    nodes = 0.5 * np.cos((np.arange(64) + 0.5) * np.pi / 128)
    powers = np.stack([nodes, nodes**3, nodes**5], axis=1)
    wanted = 2.0**0.75 * np.sin(0.5 * np.pi * nodes)
    return [float(c) for c in np.linalg.lstsq(powers, wanted, rcond=None)[0]]


C0, C1, C2 = half_turn_coefficients()


def group_members(mesh, bit):
    n_rows, n_cols = mesh.shape["sx"], mesh.shape["sy"]
    step = 1 << bit
    groups = []
    for row in range(n_rows):
        for col in range(n_cols):
            if not row & step and not col & step:
                groups.append(
                    [(row + a) * n_cols + col + c for a in (0, step) for c in (0, step)]
                )
    return groups


def fetch(pairs, sems):
    copies = [pltpu.make_async_copy(a, b, sems.at[i]) for i, (a, b) in enumerate(pairs)]
    for copy in copies:
        copy.start()
    return copies


def own_position(level):
    step = 1 << level
    row = lax.axis_index("sx") // step % 2
    col = lax.axis_index("sy") // step % 2
    return 2 * row + col


def prepare(sources, rows, cols, tables):
    a_ref, b_ref, row_ref, col_ref = tables
    lane = lax.broadcasted_iota(jnp.int32, (CHEB, NODES), 1)
    node = lax.broadcasted_iota(jnp.int32, (CHEB, NODES), 0)
    outer = (lane // CHEB == node).astype(jnp.float32)
    inner = (lane % CHEB == node).astype(jnp.float32)
    spread = functools.partial(
        lax.dot_general,
        dimension_numbers=(((0,), (0,)), ((), ())),
        precision=lax.Precision.HIGHEST,
        preferred_element_type=jnp.float32,
    )
    for bit in range(2):
        row_ref[bit] = spread(rows[bit], outer)
        col_ref[bit] = spread(cols[bit], inner)
    lines = []
    for box in range(BOXES):
        freq = sources[0, box]
        slow = sources[1, box]
        near = 16.0 * freq * freq
        lines += [near, near * slow * slow]
    columns = jnp.concatenate(lines + lines, axis=0).T
    for box in range(BOXES):
        a_ref[box] = jnp.broadcast_to(columns[:, 2 * box : 2 * box + 1], (NODES, 128))
        b_ref[box] = jnp.broadcast_to(columns[:, 2 * box + 1 : 2 * box + 2], (NODES, 128))


def weigh(position, box, targets, tables, high, low):
    a_ref, b_ref, row_ref, col_ref = tables
    row_bit, col_bit = position // 2, position % 2
    tau = targets[0, row_bit, col_bit, box]
    off = targets[1, row_bit, col_bit, box]
    tau2, off2 = tau * tau, off * off
    inner = col_ref[col_bit]
    for step in range(CHEB):
        down = pl.ds(step * CHEB, CHEB)
        along = pl.ds(NODES + step * CHEB, CHEB)
        near = a_ref[box, down, :]
        far = b_ref[box, down, :]
        near = jnp.concatenate([near, near], axis=1)
        far = jnp.concatenate([far, far], axis=1)
        kron = row_ref[row_bit, pl.ds(step, 1), :] * inner
        z = near * tau2 + far * off2
        turns = z * lax.rsqrt(z)
        rest = turns - jnp.round(turns)
        y = rest * rest
        half = rest * (C0 + y * (C1 + y * C2))
        q = half * half
        cosine = ROOT2 - q
        v = 2.0 * ROOT2 - q
        sine = half * (v * lax.rsqrt(v))
        part = kron * sine
        real = kron - part * sine
        imag = part * cosine
        for where, value in ((down, real), (along, imag)):
            top = value.astype(jnp.bfloat16)
            high[where, :] = top
            low[where, :] = (value - top.astype(jnp.float32)).astype(jnp.bfloat16)


def stacked(values):
    def turned(x):
        return jnp.concatenate([-x[RHS:], x[:RHS]], axis=0)

    top = values.astype(jnp.bfloat16)
    rest = (values - top.astype(jnp.float32)).astype(jnp.bfloat16)
    left = jnp.concatenate([top, rest], axis=0)
    right = jnp.concatenate([turned(top), turned(rest)], axis=0)
    return jnp.concatenate([left, right], axis=1)


def stack_boxes(real, imag, left):
    for box in range(BOXES):
        left[box] = stacked(jnp.concatenate([real[box], imag[box]], axis=0))


def product(left, high, low):
    main = jnp.dot(left, high, preferred_element_type=jnp.float32)
    small = jnp.dot(left[: 2 * RHS], low, preferred_element_type=jnp.float32)
    return main[: 2 * RHS] + main[2 * RHS :] + small


def put(out, index, box, total):
    out[index, 0, box] = total[:RHS]
    out[index, 1, box] = total[RHS:]


def first_kernel(
    coeffs_hbm, sources_hbm, targets_hbm, rows_hbm, cols_hbm, out_hbm,
    coeffs, sources, targets, rows, cols, *rest,
):
    *tables, high, low, left, stage, in_sems, out_sems = rest
    nodes = fetch(
        [
            (sources_hbm.at[0], sources),
            (rows_hbm.at[0], rows),
            (cols_hbm.at[0], cols),
            (targets_hbm.at[0], targets),
            (coeffs_hbm, coeffs),
        ],
        in_sems,
    )
    me = own_position(0)
    for copy in nodes[:3]:
        copy.wait()
    prepare(sources, rows, cols, tables)
    for copy in nodes[3:]:
        copy.wait()
    stack_boxes(coeffs[0], coeffs[1], left)

    def make(item):
        slot = item % 2
        weigh(me ^ (item // 2 + 1), item % 2, targets, tables, high.at[slot], low.at[slot])

    def use(item):
        slot = item % 2
        put(stage, item // 2, item % 2, product(left[item % 2], high[slot], low[slot]))

    make(0)

    def both(item, carry):
        use(item - 1)
        make(item)
        return carry

    lax.fori_loop(1, ITEMS, both, 0)
    use(ITEMS - 1)
    sent = fetch([(stage.at[x], out_hbm.at[me ^ (x + 1)]) for x in range(FOREIGN)], out_sems)
    for copy in sent:
        copy.wait()


def between_kernel(
    level, values, sources_hbm, targets_hbm, rows_hbm, cols_hbm, own, high, low,
    sources, targets, rows, cols, *rest,
):
    *tables, own_high, own_low, left, sems = rest
    last = level == LEVELS
    count = 1 if last else 2
    here = pl.ds(level - 1, count)
    nodes = fetch(
        [
            (sources_hbm.at[here], sources),
            (rows_hbm.at[here], rows),
            (cols_hbm.at[here], cols),
            (targets_hbm.at[here], targets),
        ],
        sems,
    )
    stack_boxes(values[0], values[1], left)
    for copy in nodes:
        copy.wait()
    prepare(sources.at[0], rows.at[0], cols.at[0], tables)
    me = own_position(level - 1)

    def mine(box, carry):
        weigh(me, box, targets.at[0], tables, own_high, own_low)
        total = product(left[box], own_high[...], own_low[...])
        own[0, box] = total[:RHS]
        own[1, box] = total[RHS:]
        return carry

    lax.fori_loop(0, BOXES, mine, 0)
    if last:
        return
    prepare(sources.at[1], rows.at[1], cols.at[1], tables)
    there = own_position(level)

    def make(item, carry):
        weigh(
            there ^ (item // 2 + 1), item % 2, targets.at[1], tables, high.at[item], low.at[item]
        )
        return carry

    lax.fori_loop(0, ITEMS, make, 0)


def last_between_kernel(values, sources, targets, rows, cols, own, *rest):
    between_kernel(LEVELS, values, sources, targets, rows, cols, own, None, None, *rest)


def summed(level, pieces, own):
    me = own_position(level)
    return (own[...] + pieces[me ^ 1]) + (pieces[me ^ 2] + pieces[me ^ 3])


def later_kernel(level, pieces, own, high, low, out_hbm, current, left, stage, sems):
    values = summed(level - 1, pieces, own)
    current[...] = values
    stack_boxes(values[0], values[1], left)
    me = own_position(level)
    sent = []
    for x in range(FOREIGN):
        for box in range(BOXES):
            item = 2 * x + box
            put(stage, x, box, product(left[box], high[item], low[item]))
        copy = pltpu.make_async_copy(stage.at[x], out_hbm.at[me ^ (x + 1)], sems.at[x])
        copy.start()
        sent.append(copy)
    for copy in sent:
        copy.wait()


def final_kernel(pieces, own, out):
    out[...] = summed(LEVELS - 1, pieces, own)


def node_buffers(count):
    lead = () if count is None else (count,)
    return (
        pltpu.VMEM(lead + (2, BOXES, 1, NODES), jnp.float32),
        pltpu.VMEM(lead + (2, 2, 2, BOXES, 1, NODES), jnp.float32),
        pltpu.VMEM(lead + (2, CHEB, CHEB), jnp.float32),
        pltpu.VMEM(lead + (2, CHEB, CHEB), jnp.float32),
    )


TABLES = (
    pltpu.VMEM((BOXES, NODES, 128), jnp.float32),
    pltpu.VMEM((BOXES, NODES, 128), jnp.float32),
    pltpu.VMEM((2, CHEB, NODES), jnp.float32),
    pltpu.VMEM((2, CHEB, NODES), jnp.float32),
)
FIELD = (2, BOXES, RHS, NODES)
LEFT = pltpu.VMEM((BOXES, 4 * RHS, 2 * NODES), jnp.bfloat16)
STAGE = pltpu.VMEM((FOREIGN,) + FIELD, jnp.float32)
ANY = pl.BlockSpec(memory_space=pltpu.HBM)
WHOLE = pl.BlockSpec(memory_space=pltpu.VMEM)
PARAMS = pltpu.CompilerParams(vmem_limit_bytes=12 * 1024 * 1024)


SENT = pltpu.HBM((4,) + FIELD, jnp.float32)
KEPT = pltpu.VMEM(FIELD, jnp.float32)
MADE = pltpu.VMEM((ITEMS, 2 * NODES, NODES), jnp.bfloat16)


def far(x):
    return pltpu.with_memory_space_constraint(x, pltpu.HBM)


def cost(flops):
    return pl.CostEstimate(flops=flops, bytes_accessed=100_000, transcendentals=0)


def solution(mesh):
    groups = [group_members(mesh, bit) for bit in range(LEVELS)]

    def exchange(sent, level):
        return lax.all_to_all(
            sent, ("sx", "sy"), 0, 0, axis_index_groups=groups[level], tiled=True
        )

    def local(coeffs, source_nodes, target_nodes, interp_rows, interp_cols):
        current = coeffs.reshape(FIELD)
        nodes = (
            far(source_nodes.reshape(LEVELS, 2, BOXES, 1, NODES)),
            far(target_nodes.reshape(LEVELS, 2, 2, 2, BOXES, 1, NODES)),
            far(interp_rows),
            far(interp_cols),
        )
        sent = pl.pallas_call(
            first_kernel,
            in_specs=[ANY] * 5,
            out_specs=ANY,
            out_shape=SENT,
            scratch_shapes=(pltpu.VMEM(FIELD, jnp.float32),)
            + node_buffers(None)
            + TABLES
            + (pltpu.VMEM((2, 2 * NODES, NODES), jnp.bfloat16),) * 2
            + (LEFT, STAGE, pltpu.SemaphoreType.DMA((5,)), pltpu.SemaphoreType.DMA((FOREIGN,))),
            compiler_params=PARAMS,
            name="first",
        )(far(current), *nodes)
        for level in range(1, LEVELS + 1):
            last = level == LEVELS
            made = pl.pallas_call(
                last_between_kernel if last else functools.partial(between_kernel, level),
                in_specs=[WHOLE] + [ANY] * 4,
                out_specs=[WHOLE] * (1 if last else 3),
                out_shape=[KEPT] + ([] if last else [MADE] * 2),
                scratch_shapes=node_buffers(1 if last else 2)
                + TABLES
                + (pltpu.VMEM((2 * NODES, NODES), jnp.bfloat16),) * 2
                + (LEFT, pltpu.SemaphoreType.DMA((4,))),
                compiler_params=PARAMS,
                cost_estimate=cost(60_000_000),
                name=f"between_{level}",
            )(current, *nodes)
            pieces = exchange(sent, level - 1)
            if last:
                break
            sent, current = pl.pallas_call(
                functools.partial(later_kernel, level),
                in_specs=[WHOLE] * 4,
                out_specs=[ANY, WHOLE],
                out_shape=[SENT, KEPT],
                scratch_shapes=(LEFT, STAGE, pltpu.SemaphoreType.DMA((FOREIGN,))),
                compiler_params=PARAMS,
                name=f"later_{level}",
            )(pieces, *made)
        field = pl.pallas_call(
            final_kernel,
            in_specs=[WHOLE] * 2,
            out_specs=WHOLE,
            out_shape=jax.ShapeDtypeStruct(FIELD, jnp.float32),
            compiler_params=PARAMS,
            name="final",
        )(pieces, *made)
        return field.reshape(2, BOXES, 1, RHS, NODES)

    in_specs = (
        P(None, "sx", "sy", None, None),
        P(None, None, "sx", "sy", None),
        P(None, None, None, None, "sx", "sy", None),
        P(),
        P(),
    )
    out_specs = P(None, "sx", "sy", None, None)
    return jax.shard_map(local, mesh=mesh, in_specs=in_specs, out_specs=out_specs, check_vma=False)
```

```python
import functools
import math

import jax
import jax.numpy as jnp
import numpy as np
from jax import lax
from jax.experimental import pallas as pl
from jax.experimental.pallas import tpu as pltpu
from jax.sharding import PartitionSpec as P

LEVELS = 3
CHEB = 16
NODES = CHEB * CHEB
RHS = 16
BOXES = 2
FOREIGN = 3
ITEMS = FOREIGN * BOXES
ROOT2 = math.sqrt(2.0)
SOURCE_LINE = 2 * BOXES * RHS
TARGET_LINE = SOURCE_LINE + 2 * BOXES
PACKED = 88


def half_turn_coefficients():
    nodes = 0.5 * np.cos((np.arange(64) + 0.5) * np.pi / 128)
    powers = np.stack([nodes, nodes**3, nodes**5], axis=1)
    wanted = 2.0**0.75 * np.sin(0.5 * np.pi * nodes)
    return [float(c) for c in np.linalg.lstsq(powers, wanted, rcond=None)[0]]


C0, C1, C2 = half_turn_coefficients()


def group_members(mesh, bit):
    n_rows, n_cols = mesh.shape["sx"], mesh.shape["sy"]
    step = 1 << bit
    groups = []
    for row in range(n_rows):
        for col in range(n_cols):
            if not row & step and not col & step:
                groups.append(
                    [(row + a) * n_cols + col + c for a in (0, step) for c in (0, step)]
                )
    return groups


def swapped(block, axis):
    count = lax.axis_size(axis)
    return lax.ppermute(block, axis, [(i, i ^ 1) for i in range(count)])


def fetch(pairs, sems):
    copies = [pltpu.make_async_copy(a, b, sems.at[i]) for i, (a, b) in enumerate(pairs)]
    for copy in copies:
        copy.start()
    return copies


def own_position(level):
    step = 1 << level
    row = lax.axis_index("sx") // step % 2
    col = lax.axis_index("sy") // step % 2
    return 2 * row + col


def spread_matrices(rows, cols, row_ref, col_ref):
    lane = lax.broadcasted_iota(jnp.int32, (CHEB, NODES), 1)
    node = lax.broadcasted_iota(jnp.int32, (CHEB, NODES), 0)
    outer = (lane // CHEB == node).astype(jnp.float32)
    inner = (lane % CHEB == node).astype(jnp.float32)
    spread = functools.partial(
        lax.dot_general,
        dimension_numbers=(((0,), (0,)), ((), ())),
        precision=lax.Precision.HIGHEST,
        preferred_element_type=jnp.float32,
    )
    for bit in range(2):
        row_ref[bit] = spread(rows[bit], outer)
        col_ref[bit] = spread(cols[bit], inner)


def spread_sources(source, a_ref, b_ref):
    lines = []
    for box in range(BOXES):
        freq = source(0, box)
        slow = source(1, box)
        near = 16.0 * freq * freq
        lines += [near, near * slow * slow]
    columns = jnp.concatenate(lines + lines, axis=0).T
    for box in range(BOXES):
        a_ref[box] = jnp.broadcast_to(columns[:, 2 * box : 2 * box + 1], (NODES, 128))
        b_ref[box] = jnp.broadcast_to(columns[:, 2 * box + 1 : 2 * box + 2], (NODES, 128))


def prepare(sources, rows, cols, tables):
    a_ref, b_ref, row_ref, col_ref = tables
    spread_matrices(rows, cols, row_ref, col_ref)
    spread_sources(lambda kind, box: sources[kind, box], a_ref, b_ref)


def line_of(targets):
    return lambda kind, row_bit, col_bit, box: targets[kind, row_bit, col_bit, box]


def weigh(position, box, target, tables, high, low):
    a_ref, b_ref, row_ref, col_ref = tables
    row_bit, col_bit = position // 2, position % 2
    tau = target(0, row_bit, col_bit, box)
    off = target(1, row_bit, col_bit, box)
    tau2, off2 = tau * tau, off * off
    inner = col_ref[col_bit]
    for step in range(CHEB):
        down = pl.ds(step * CHEB, CHEB)
        along = pl.ds(NODES + step * CHEB, CHEB)
        near = a_ref[box, down, :]
        far = b_ref[box, down, :]
        near = jnp.concatenate([near, near], axis=1)
        far = jnp.concatenate([far, far], axis=1)
        kron = row_ref[row_bit, pl.ds(step, 1), :] * inner
        z = near * tau2 + far * off2
        turns = z * lax.rsqrt(z)
        rest = turns - jnp.round(turns)
        y = rest * rest
        half = rest * (C0 + y * (C1 + y * C2))
        q = half * half
        cosine = ROOT2 - q
        v = 2.0 * ROOT2 - q
        sine = half * (v * lax.rsqrt(v))
        part = kron * sine
        real = kron - part * sine
        imag = part * cosine
        for where, value in ((down, real), (along, imag)):
            top = value.astype(jnp.bfloat16)
            high[where, :] = top
            low[where, :] = (value - top.astype(jnp.float32)).astype(jnp.bfloat16)


def stacked(values):
    def turned(x):
        return jnp.concatenate([-x[RHS:], x[:RHS]], axis=0)

    top = values.astype(jnp.bfloat16)
    rest = (values - top.astype(jnp.float32)).astype(jnp.bfloat16)
    left = jnp.concatenate([top, rest], axis=0)
    right = jnp.concatenate([turned(top), turned(rest)], axis=0)
    return jnp.concatenate([left, right], axis=1)


def stack_boxes(real, imag, left):
    for box in range(BOXES):
        left[box] = stacked(jnp.concatenate([real[box], imag[box]], axis=0))


def product(left, high, low):
    main = jnp.dot(left, high, preferred_element_type=jnp.float32)
    small = jnp.dot(left[: 2 * RHS], low, preferred_element_type=jnp.float32)
    return main[: 2 * RHS] + main[2 * RHS :] + small


def put(out, index, box, total):
    out[index, 0, box] = total[:RHS]
    out[index, 1, box] = total[RHS:]


def packed_source(packed):
    return lambda kind, box: packed[pl.ds(SOURCE_LINE + 2 * kind + box, 1), :]


def packed_target(packed):
    def line(kind, row_bit, col_bit, box):
        place = ((kind * 2 + row_bit) * 2 + col_bit) * BOXES + box
        return packed[pl.ds(TARGET_LINE + place, 1), :]

    return line


def packed_values(packed, box):
    real = packed[box * RHS : (box + 1) * RHS, :]
    imag = packed[(BOXES + box) * RHS : (BOXES + box + 1) * RHS, :]
    return jnp.concatenate([real, imag], axis=0)


def pack_kernel(
    coeffs_hbm, sources_hbm, targets_hbm, rows_hbm, cols_hbm, packed, rows, cols,
    coeffs, sources, targets, sems,
):
    copies = fetch(
        [
            (coeffs_hbm, coeffs),
            (sources_hbm.at[0], sources),
            (targets_hbm.at[0], targets),
            (rows_hbm.at[0], rows),
            (cols_hbm.at[0], cols),
        ],
        sems,
    )
    for copy in copies:
        copy.wait()
    for part in range(2):
        for box in range(BOXES):
            packed[pl.ds((part * BOXES + box) * RHS, RHS), :] = coeffs[part, box]
    lines = [sources[kind, box] for kind in range(2) for box in range(BOXES)]
    for kind in range(2):
        for place in range(4 * BOXES):
            lines.append(targets[kind, place // 4, place // 2 % 2, place % 2])
    lines += [lines[-1]] * (PACKED - SOURCE_LINE - len(lines))
    packed[pl.ds(SOURCE_LINE, PACKED - SOURCE_LINE), :] = jnp.concatenate(lines, axis=0)


def pair_of_boxes(packed, position, tables, high, low):
    target = packed_target(packed)
    for box in range(BOXES):
        weigh(position, box, target, tables, high.at[box], low.at[box])
    return [
        product(stacked(packed_values(packed, box)), high[box], low[box]) for box in range(BOXES)
    ]


def near_kernel(packed, rows, cols, partial, row_ref, col_ref, a_ref, b_ref, high, low):
    spread_matrices(rows, cols, row_ref, col_ref)
    spread_sources(packed_source(packed), a_ref, b_ref)
    tables = (a_ref, b_ref, row_ref, col_ref)
    both = pair_of_boxes(packed, own_position(0) ^ 2, tables, high, low)
    for box in range(BOXES):
        partial[0, box] = both[box][:RHS]
        partial[1, box] = both[box][RHS:]


def partner_kernel(packed, row_ref, col_ref, partial, sent, a_ref, b_ref, high, low):
    spread_sources(packed_source(packed), a_ref, b_ref)
    tables = (a_ref, b_ref, row_ref, col_ref)
    both = pair_of_boxes(packed, own_position(0) ^ 2, tables, high, low)
    for box in range(BOXES):
        sent[0, box] = partial[0, box] + both[box][:RHS]
        sent[1, box] = partial[1, box] + both[box][RHS:]


def foreign_weights(level, targets, tables, high, low):
    there = own_position(level)

    def make(item, carry):
        weigh(
            there ^ (item // 2 + 1), item % 2, line_of(targets), tables, high.at[item], low.at[item]
        )
        return carry

    lax.fori_loop(0, ITEMS, make, 0)


def second_kernel(
    packed, got, row0_ref, col0_ref, sources_hbm, targets_hbm, rows_hbm, cols_hbm, own, high, low,
    sources, targets, rows, cols, *rest,
):
    a_ref, b_ref, row_ref, col_ref, own_high, own_low, sems = rest
    nodes = fetch(
        [
            (sources_hbm.at[1], sources),
            (rows_hbm.at[1], rows),
            (cols_hbm.at[1], cols),
            (targets_hbm.at[1], targets),
        ],
        sems,
    )
    me = own_position(0)
    tables = (a_ref, b_ref, row0_ref, col0_ref)
    for index, lines in enumerate((packed, got)):
        spread_sources(packed_source(lines), a_ref, b_ref)

        def mine(box, carry):
            weigh(me, box, packed_target(lines), tables, own_high, own_low)
            start = pl.multiple_of(box * RHS, RHS)
            real = lines[pl.ds(start, RHS), :]
            imag = lines[pl.ds(start + BOXES * RHS, RHS), :]
            left = stacked(jnp.concatenate([real, imag], axis=0))
            total = product(left, own_high[...], own_low[...])
            if index:
                own[0, box] += total[:RHS]
                own[1, box] += total[RHS:]
            else:
                own[0, box] = total[:RHS]
                own[1, box] = total[RHS:]
            return carry

        lax.fori_loop(0, BOXES, mine, 0)
    for copy in nodes:
        copy.wait()
    tables = (a_ref, b_ref, row_ref, col_ref)
    prepare(sources, rows, cols, tables)
    foreign_weights(1, targets, tables, high, low)


def between_kernel(
    level, values, sources_hbm, targets_hbm, rows_hbm, cols_hbm, own, high, low,
    sources, targets, rows, cols, *rest,
):
    *tables, own_high, own_low, left, sems = rest
    last = level == LEVELS
    count = 1 if last else 2
    here = pl.ds(level - 1, count)
    nodes = fetch(
        [
            (sources_hbm.at[here], sources),
            (rows_hbm.at[here], rows),
            (cols_hbm.at[here], cols),
            (targets_hbm.at[here], targets),
        ],
        sems,
    )
    stack_boxes(values[0], values[1], left)
    for copy in nodes:
        copy.wait()
    prepare(sources.at[0], rows.at[0], cols.at[0], tables)
    me = own_position(level - 1)

    def mine(box, carry):
        weigh(me, box, line_of(targets.at[0]), tables, own_high, own_low)
        total = product(left[box], own_high[...], own_low[...])
        own[0, box] = total[:RHS]
        own[1, box] = total[RHS:]
        return carry

    lax.fori_loop(0, BOXES, mine, 0)
    if last:
        return
    prepare(sources.at[1], rows.at[1], cols.at[1], tables)
    foreign_weights(level, targets.at[1], tables, high, low)


def last_between_kernel(values, sources, targets, rows, cols, own, *rest):
    between_kernel(LEVELS, values, sources, targets, rows, cols, own, None, None, *rest)


def summed(level, pieces, own):
    me = own_position(level)
    return (own[...] + pieces[me ^ 1]) + (pieces[me ^ 2] + pieces[me ^ 3])


def later_kernel(level, pieces, own, high, low, out_hbm, current, left, stage, sems):
    if level == 1:
        values = own[...] + pieces[...]
    else:
        values = summed(level - 1, pieces, own)
    current[...] = values
    stack_boxes(values[0], values[1], left)
    me = own_position(level)
    sent = []
    for x in range(FOREIGN):
        for box in range(BOXES):
            item = 2 * x + box
            put(stage, x, box, product(left[box], high[item], low[item]))
        copy = pltpu.make_async_copy(stage.at[x], out_hbm.at[me ^ (x + 1)], sems.at[x])
        copy.start()
        sent.append(copy)
    for copy in sent:
        copy.wait()


def final_kernel(pieces, own, out):
    out[...] = summed(LEVELS - 1, pieces, own)


def node_buffers(count):
    lead = () if count is None else (count,)
    return (
        pltpu.VMEM(lead + (2, BOXES, 1, NODES), jnp.float32),
        pltpu.VMEM(lead + (2, 2, 2, BOXES, 1, NODES), jnp.float32),
        pltpu.VMEM(lead + (2, CHEB, CHEB), jnp.float32),
        pltpu.VMEM(lead + (2, CHEB, CHEB), jnp.float32),
    )


TABLES = (
    pltpu.VMEM((BOXES, NODES, 128), jnp.float32),
    pltpu.VMEM((BOXES, NODES, 128), jnp.float32),
    pltpu.VMEM((2, CHEB, NODES), jnp.float32),
    pltpu.VMEM((2, CHEB, NODES), jnp.float32),
)
FIELD = (2, BOXES, RHS, NODES)
LEFT = pltpu.VMEM((BOXES, 4 * RHS, 2 * NODES), jnp.bfloat16)
STAGE = pltpu.VMEM((FOREIGN,) + FIELD, jnp.float32)
ANY = pl.BlockSpec(memory_space=pltpu.HBM)
WHOLE = pl.BlockSpec(memory_space=pltpu.VMEM)
PARAMS = pltpu.CompilerParams(vmem_limit_bytes=12 * 1024 * 1024)


SENT = pltpu.HBM((4,) + FIELD, jnp.float32)
KEPT = pltpu.VMEM(FIELD, jnp.float32)
SPREAD = pltpu.VMEM((2, CHEB, NODES), jnp.float32)
SMALL = pltpu.VMEM((2, CHEB, CHEB), jnp.float32)
ONE = pltpu.VMEM((2 * NODES, NODES), jnp.bfloat16)
PAIR = pltpu.VMEM((BOXES, 2 * NODES, NODES), jnp.bfloat16)
COLUMNS = pltpu.VMEM((BOXES, NODES, 128), jnp.float32)
MADE = pltpu.VMEM((ITEMS, 2 * NODES, NODES), jnp.bfloat16)


def far(x):
    return pltpu.with_memory_space_constraint(x, pltpu.HBM)


def cost(flops):
    return pl.CostEstimate(flops=flops, bytes_accessed=100_000, transcendentals=0)


def solution(mesh):
    groups = [group_members(mesh, bit) for bit in range(LEVELS)]

    def exchange(sent, level):
        return lax.all_to_all(
            sent, ("sx", "sy"), 0, 0, axis_index_groups=groups[level], tiled=True
        )

    def local(coeffs, source_nodes, target_nodes, interp_rows, interp_cols):
        current = coeffs.reshape(FIELD)
        nodes = (
            far(source_nodes.reshape(LEVELS, 2, BOXES, 1, NODES)),
            far(target_nodes.reshape(LEVELS, 2, 2, 2, BOXES, 1, NODES)),
            far(interp_rows),
            far(interp_cols),
        )
        packed, rows, cols = pl.pallas_call(
            pack_kernel,
            in_specs=[ANY] * 5,
            out_specs=[WHOLE] * 3,
            out_shape=[pltpu.VMEM((PACKED, NODES), jnp.float32), SMALL, SMALL],
            scratch_shapes=(KEPT,) + node_buffers(None)[:2] + (pltpu.SemaphoreType.DMA((5,)),),
            compiler_params=PARAMS,
            name="pack",
        )(far(current), *nodes)
        got = swapped(packed, "sy")
        partial, row0, col0 = pl.pallas_call(
            near_kernel,
            in_specs=[WHOLE] * 3,
            out_specs=[WHOLE] * 3,
            out_shape=[KEPT, SPREAD, SPREAD],
            scratch_shapes=(COLUMNS, COLUMNS, PAIR, PAIR),
            compiler_params=PARAMS,
            cost_estimate=cost(20_000_000),
            name="near",
        )(packed, rows, cols)
        sent = pl.pallas_call(
            partner_kernel,
            in_specs=[WHOLE] * 4,
            out_specs=WHOLE,
            out_shape=KEPT,
            scratch_shapes=(COLUMNS, COLUMNS, PAIR, PAIR),
            compiler_params=PARAMS,
            name="partner",
        )(got, row0, col0, partial)
        made = pl.pallas_call(
            second_kernel,
            in_specs=[WHOLE] * 4 + [ANY] * 4,
            out_specs=[WHOLE] * 3,
            out_shape=[KEPT, MADE, MADE],
            scratch_shapes=node_buffers(None)
            + (COLUMNS, COLUMNS, SPREAD, SPREAD, ONE, ONE, pltpu.SemaphoreType.DMA((4,))),
            compiler_params=PARAMS,
            cost_estimate=cost(60_000_000),
            name="second",
        )(packed, got, row0, col0, *nodes)
        pieces = swapped(sent, "sx")
        for level in range(1, LEVELS):
            sent, current = pl.pallas_call(
                functools.partial(later_kernel, level),
                in_specs=[WHOLE] * 4,
                out_specs=[ANY, WHOLE],
                out_shape=[SENT, KEPT],
                scratch_shapes=(LEFT, STAGE, pltpu.SemaphoreType.DMA((FOREIGN,))),
                compiler_params=PARAMS,
                name=f"later_{level}",
            )(pieces, *made)
            last = level + 1 == LEVELS
            made = pl.pallas_call(
                last_between_kernel if last else functools.partial(between_kernel, level + 1),
                in_specs=[WHOLE] + [ANY] * 4,
                out_specs=[WHOLE] * (1 if last else 3),
                out_shape=[KEPT] + ([] if last else [MADE] * 2),
                scratch_shapes=node_buffers(1 if last else 2)
                + TABLES
                + (ONE, ONE, LEFT, pltpu.SemaphoreType.DMA((4,))),
                compiler_params=PARAMS,
                cost_estimate=cost(60_000_000),
                name=f"between_{level + 1}",
            )(current, *nodes)
            pieces = exchange(sent, level)
        field = pl.pallas_call(
            final_kernel,
            in_specs=[WHOLE] * 2,
            out_specs=WHOLE,
            out_shape=jax.ShapeDtypeStruct(FIELD, jnp.float32),
            compiler_params=PARAMS,
            name="final",
        )(pieces, *made)
        return field.reshape(2, BOXES, 1, RHS, NODES)

    in_specs = (
        P(None, "sx", "sy", None, None),
        P(None, None, "sx", "sy", None),
        P(None, None, None, None, "sx", "sy", None),
        P(),
        P(),
    )
    out_specs = P(None, "sx", "sy", None, None)
    return jax.shard_map(local, mesh=mesh, in_specs=in_specs, out_specs=out_specs, check_vma=False)
```

```python
import functools
import math

import jax
import jax.numpy as jnp
import numpy as np
from jax import lax
from jax.experimental import pallas as pl
from jax.experimental.pallas import tpu as pltpu
from jax.sharding import PartitionSpec as P

LEVELS = 3
CHEB = 16
NODES = CHEB * CHEB
RHS = 16
BOXES = 2
FOREIGN = 3
ITEMS = FOREIGN * BOXES
ROOT2 = math.sqrt(2.0)
SOURCE_LINE = 2 * BOXES * RHS
TARGET_LINE = SOURCE_LINE + 2 * BOXES
PACKED = 88
LOW_SCALE = 2.0**17


def half_turn_coefficients():
    nodes = 0.5 * np.cos((np.arange(64) + 0.5) * np.pi / 128)
    powers = np.stack([nodes, nodes**3, nodes**5], axis=1)
    wanted = 2.0**0.75 * np.sin(0.5 * np.pi * nodes)
    return [float(c) for c in np.linalg.lstsq(powers, wanted, rcond=None)[0]]


C0, C1, C2 = half_turn_coefficients()


def group_members(mesh, bit):
    n_rows, n_cols = mesh.shape["sx"], mesh.shape["sy"]
    step = 1 << bit
    groups = []
    for row in range(n_rows):
        for col in range(n_cols):
            if not row & step and not col & step:
                groups.append(
                    [(row + a) * n_cols + col + c for a in (0, step) for c in (0, step)]
                )
    return groups


def swapped(block, axis):
    count = lax.axis_size(axis)
    return lax.ppermute(block, axis, [(i, i ^ 1) for i in range(count)])


def fetch(pairs, sems):
    copies = [pltpu.make_async_copy(a, b, sems.at[i]) for i, (a, b) in enumerate(pairs)]
    for copy in copies:
        copy.start()
    return copies


def own_position(level):
    step = 1 << level
    row = lax.axis_index("sx") // step % 2
    col = lax.axis_index("sy") // step % 2
    return 2 * row + col


def spread_matrices(rows, cols, row_ref, col_ref):
    lane = lax.broadcasted_iota(jnp.int32, (CHEB, NODES), 1)
    node = lax.broadcasted_iota(jnp.int32, (CHEB, NODES), 0)
    outer = (lane // CHEB == node).astype(jnp.float32)
    inner = (lane % CHEB == node).astype(jnp.float32)
    spread = functools.partial(
        lax.dot_general,
        dimension_numbers=(((0,), (0,)), ((), ())),
        precision=lax.Precision.HIGHEST,
        preferred_element_type=jnp.float32,
    )
    for bit in range(2):
        row_ref[bit] = spread(rows[bit], outer)
        col_ref[bit] = spread(cols[bit], inner)


def spread_sources(source, a_ref, b_ref):
    lines = []
    for box in range(BOXES):
        freq = source(0, box)
        slow = source(1, box)
        near = 16.0 * freq * freq
        lines += [near, near * slow * slow]
    columns = jnp.concatenate(lines + lines, axis=0).T
    for box in range(BOXES):
        a_ref[box] = jnp.broadcast_to(columns[:, 2 * box : 2 * box + 1], (NODES, 128))
        b_ref[box] = jnp.broadcast_to(columns[:, 2 * box + 1 : 2 * box + 2], (NODES, 128))


def prepare(sources, rows, cols, tables):
    a_ref, b_ref, row_ref, col_ref = tables
    spread_matrices(rows, cols, row_ref, col_ref)
    spread_sources(lambda kind, box: sources[kind, box], a_ref, b_ref)


def line_of(targets):
    return lambda kind, row_bit, col_bit, box: targets[kind, row_bit, col_bit, box]


def weigh(position, box, target, tables, high, low):
    a_ref, b_ref, row_ref, col_ref = tables
    row_bit, col_bit = position // 2, position % 2
    tau = target(0, row_bit, col_bit, box)
    off = target(1, row_bit, col_bit, box)
    tau2, off2 = tau * tau, off * off
    inner = col_ref[col_bit]
    for step in range(CHEB):
        down = pl.ds(step * CHEB, CHEB)
        along = pl.ds(NODES + step * CHEB, CHEB)
        near = a_ref[box, down, :]
        far = b_ref[box, down, :]
        near = jnp.concatenate([near, near], axis=1)
        far = jnp.concatenate([far, far], axis=1)
        kron = row_ref[row_bit, pl.ds(step, 1), :] * inner
        z = near * tau2 + far * off2
        turns = z * lax.rsqrt(z)
        rest = turns - jnp.round(turns)
        y = rest * rest
        half = rest * (C0 + y * (C1 + y * C2))
        q = half * half
        cosine = ROOT2 - q
        v = 2.0 * ROOT2 - q
        sine = half * (v * lax.rsqrt(v))
        part = kron * sine
        real = kron - part * sine
        imag = part * cosine
        for where, value in ((down, real), (along, imag)):
            top = value.astype(jnp.bfloat16)
            high[where, :] = top
            rest_of = value - top.astype(jnp.float32)
            if low.dtype != jnp.bfloat16:
                rest_of = rest_of * LOW_SCALE
            low[where, :] = rest_of.astype(low.dtype)


def stacked(values):
    def turned(x):
        return jnp.concatenate([-x[RHS:], x[:RHS]], axis=0)

    top = values.astype(jnp.bfloat16)
    rest = (values - top.astype(jnp.float32)).astype(jnp.bfloat16)
    left = jnp.concatenate([top, rest], axis=0)
    right = jnp.concatenate([turned(top), turned(rest)], axis=0)
    return jnp.concatenate([left, right], axis=1)


def stack_boxes(real, imag, left):
    for box in range(BOXES):
        left[box] = stacked(jnp.concatenate([real[box], imag[box]], axis=0))


def product(left, high, low):
    main = jnp.dot(left, high, preferred_element_type=jnp.float32)
    scaled = low.dtype != jnp.bfloat16
    small = jnp.dot(
        left[: 2 * RHS], low.astype(jnp.bfloat16), preferred_element_type=jnp.float32
    )
    if scaled:
        small = small * (1.0 / LOW_SCALE)
    return main[: 2 * RHS] + main[2 * RHS :] + small


def put(out, index, box, total):
    out[index, 0, box] = total[:RHS]
    out[index, 1, box] = total[RHS:]


def packed_source(packed):
    return lambda kind, box: packed[pl.ds(SOURCE_LINE + 2 * kind + box, 1), :]


def packed_target(packed):
    def line(kind, row_bit, col_bit, box):
        place = ((kind * 2 + row_bit) * 2 + col_bit) * BOXES + box
        return packed[pl.ds(TARGET_LINE + place, 1), :]

    return line


def packed_values(packed, box):
    real = packed[box * RHS : (box + 1) * RHS, :]
    imag = packed[(BOXES + box) * RHS : (BOXES + box + 1) * RHS, :]
    return jnp.concatenate([real, imag], axis=0)


def pack_kernel(
    coeffs_hbm, sources_hbm, targets_hbm, rows_hbm, cols_hbm, packed, rows, cols,
    coeffs, sources, targets, sems,
):
    copies = fetch(
        [
            (coeffs_hbm, coeffs),
            (sources_hbm.at[0], sources),
            (targets_hbm.at[0], targets),
            (rows_hbm.at[0], rows),
            (cols_hbm.at[0], cols),
        ],
        sems,
    )
    for copy in copies:
        copy.wait()
    for part in range(2):
        for box in range(BOXES):
            packed[pl.ds((part * BOXES + box) * RHS, RHS), :] = coeffs[part, box]
    lines = [sources[kind, box] for kind in range(2) for box in range(BOXES)]
    for kind in range(2):
        for place in range(4 * BOXES):
            lines.append(targets[kind, place // 4, place // 2 % 2, place % 2])
    lines += [lines[-1]] * (PACKED - SOURCE_LINE - len(lines))
    packed[pl.ds(SOURCE_LINE, PACKED - SOURCE_LINE), :] = jnp.concatenate(lines, axis=0)


def pair_of_boxes(packed, position, tables, high, low):
    target = packed_target(packed)
    for box in range(BOXES):
        weigh(position, box, target, tables, high.at[box], low.at[box])
    return [
        product(stacked(packed_values(packed, box)), high[box], low[box]) for box in range(BOXES)
    ]


def near_kernel(packed, rows, cols, partial, row_ref, col_ref, a_ref, b_ref, high, low):
    spread_matrices(rows, cols, row_ref, col_ref)
    spread_sources(packed_source(packed), a_ref, b_ref)
    tables = (a_ref, b_ref, row_ref, col_ref)
    both = pair_of_boxes(packed, own_position(0) ^ 2, tables, high, low)
    for box in range(BOXES):
        partial[0, box] = both[box][:RHS]
        partial[1, box] = both[box][RHS:]


def partner_kernel(packed, row_ref, col_ref, partial, sent, a_ref, b_ref, high, low):
    spread_sources(packed_source(packed), a_ref, b_ref)
    tables = (a_ref, b_ref, row_ref, col_ref)
    both = pair_of_boxes(packed, own_position(0) ^ 2, tables, high, low)
    for box in range(BOXES):
        sent[0, box] = partial[0, box] + both[box][:RHS]
        sent[1, box] = partial[1, box] + both[box][RHS:]


def make_weights(level, first, targets, tables, high, low):
    there = own_position(level)

    def make(item, carry):
        weigh(
            there ^ (item // 2 + first),
            item % 2,
            line_of(targets),
            tables,
            high.at[item],
            low.at[item],
        )
        return carry

    lax.fori_loop(0, (4 - first) * BOXES, make, 0)


def second_kernel(
    packed, got, row0_ref, col0_ref, sources_hbm, targets_hbm, rows_hbm, cols_hbm, own, high, low,
    sources, targets, rows, cols, *rest,
):
    a_ref, b_ref, row_ref, col_ref, own_high, own_low, sems = rest
    nodes = fetch(
        [
            (sources_hbm.at[1], sources),
            (rows_hbm.at[1], rows),
            (cols_hbm.at[1], cols),
            (targets_hbm.at[1], targets),
        ],
        sems,
    )
    me = own_position(0)
    tables = (a_ref, b_ref, row0_ref, col0_ref)
    for index, lines in enumerate((packed, got)):
        spread_sources(packed_source(lines), a_ref, b_ref)

        def mine(box, carry):
            weigh(me, box, packed_target(lines), tables, own_high, own_low)
            start = pl.multiple_of(box * RHS, RHS)
            real = lines[pl.ds(start, RHS), :]
            imag = lines[pl.ds(start + BOXES * RHS, RHS), :]
            left = stacked(jnp.concatenate([real, imag], axis=0))
            total = product(left, own_high[...], own_low[...])
            if index:
                own[0, box] += total[:RHS]
                own[1, box] += total[RHS:]
            else:
                own[0, box] = total[:RHS]
                own[1, box] = total[RHS:]
            return carry

        lax.fori_loop(0, BOXES, mine, 0)
    for copy in nodes:
        copy.wait()
    tables = (a_ref, b_ref, row_ref, col_ref)
    prepare(sources, rows, cols, tables)
    make_weights(1, 1, targets, tables, high, low)


def between_kernel(
    values, sources_hbm, targets_hbm, rows_hbm, cols_hbm, own, high, low,
    sources, targets, rows, cols, *rest,
):
    *tables, own_high, own_low, left, sems = rest
    here = pl.ds(1, 2)
    nodes = fetch(
        [
            (sources_hbm.at[here], sources),
            (rows_hbm.at[here], rows),
            (cols_hbm.at[here], cols),
            (targets_hbm.at[here], targets),
        ],
        sems,
    )
    stack_boxes(values[0], values[1], left)
    for copy in nodes:
        copy.wait()
    prepare(sources.at[0], rows.at[0], cols.at[0], tables)
    me = own_position(1)

    def mine(box, carry):
        weigh(me, box, line_of(targets.at[0]), tables, own_high, own_low)
        total = product(left[box], own_high[...], own_low[...])
        own[0, box] = total[:RHS]
        own[1, box] = total[RHS:]
        return carry

    lax.fori_loop(0, BOXES, mine, 0)
    prepare(sources.at[1], rows.at[1], cols.at[1], tables)
    make_weights(2, 0, targets.at[1], tables, high, low)


def middle_kernel(piece, own, high, low, out_hbm, current, left, stage, sems):
    values = own[...] + piece[...]
    current[...] = values
    stack_boxes(values[0], values[1], left)
    me = own_position(1)
    sent = []
    for x in range(FOREIGN):
        for box in range(BOXES):
            item = 2 * x + box
            put(stage, x, box, product(left[box], high[item], low[item]))
        copy = pltpu.make_async_copy(stage.at[x], out_hbm.at[me ^ (x + 1)], sems.at[x])
        copy.start()
        sent.append(copy)
    for copy in sent:
        copy.wait()


def late_kernel(pieces, own, high, low, out, left):
    me = own_position(1)
    values = (own[...] + pieces[me ^ 1]) + (pieces[me ^ 2] + pieces[me ^ 3])
    stack_boxes(values[0], values[1], left)
    there = own_position(2)
    for x in range(4):
        for box in range(BOXES):
            item = 2 * x + box
            put(out, there ^ x, box, product(left[box], high[item], low[item]))


def final_kernel(pieces, out):
    out[...] = (pieces[0] + pieces[1]) + (pieces[2] + pieces[3])


def node_buffers(count):
    lead = () if count is None else (count,)
    return (
        pltpu.VMEM(lead + (2, BOXES, 1, NODES), jnp.float32),
        pltpu.VMEM(lead + (2, 2, 2, BOXES, 1, NODES), jnp.float32),
        pltpu.VMEM(lead + (2, CHEB, CHEB), jnp.float32),
        pltpu.VMEM(lead + (2, CHEB, CHEB), jnp.float32),
    )


TABLES = (
    pltpu.VMEM((BOXES, NODES, 128), jnp.float32),
    pltpu.VMEM((BOXES, NODES, 128), jnp.float32),
    pltpu.VMEM((2, CHEB, NODES), jnp.float32),
    pltpu.VMEM((2, CHEB, NODES), jnp.float32),
)
FIELD = (2, BOXES, RHS, NODES)
LEFT = pltpu.VMEM((BOXES, 4 * RHS, 2 * NODES), jnp.bfloat16)
STAGE = pltpu.VMEM((FOREIGN,) + FIELD, jnp.float32)
ANY = pl.BlockSpec(memory_space=pltpu.HBM)
WHOLE = pl.BlockSpec(memory_space=pltpu.VMEM)
PARAMS = pltpu.CompilerParams(vmem_limit_bytes=12 * 1024 * 1024)


SENT = pltpu.HBM((4,) + FIELD, jnp.float32)
KEPT = pltpu.VMEM(FIELD, jnp.float32)
SPREAD = pltpu.VMEM((2, CHEB, NODES), jnp.float32)
SMALL = pltpu.VMEM((2, CHEB, CHEB), jnp.float32)
ONE = pltpu.VMEM((2 * NODES, NODES), jnp.bfloat16)
PAIR = pltpu.VMEM((BOXES, 2 * NODES, NODES), jnp.bfloat16)
COLUMNS = pltpu.VMEM((BOXES, NODES, 128), jnp.float32)
MADE = pltpu.VMEM((ITEMS, 2 * NODES, NODES), jnp.bfloat16)


def far(x):
    return pltpu.with_memory_space_constraint(x, pltpu.HBM)


def cost(flops):
    return pl.CostEstimate(flops=flops, bytes_accessed=100_000, transcendentals=0)


def solution(mesh):
    groups = [group_members(mesh, bit) for bit in range(LEVELS)]

    def exchange(sent, level):
        return lax.all_to_all(
            sent, ("sx", "sy"), 0, 0, axis_index_groups=groups[level], tiled=True
        )

    def local(coeffs, source_nodes, target_nodes, interp_rows, interp_cols):
        current = coeffs.reshape(FIELD)
        nodes = (
            far(source_nodes.reshape(LEVELS, 2, BOXES, 1, NODES)),
            far(target_nodes.reshape(LEVELS, 2, 2, 2, BOXES, 1, NODES)),
            far(interp_rows),
            far(interp_cols),
        )
        packed, rows, cols = pl.pallas_call(
            pack_kernel,
            in_specs=[ANY] * 5,
            out_specs=[WHOLE] * 3,
            out_shape=[pltpu.VMEM((PACKED, NODES), jnp.float32), SMALL, SMALL],
            scratch_shapes=(KEPT,) + node_buffers(None)[:2] + (pltpu.SemaphoreType.DMA((5,)),),
            compiler_params=PARAMS,
            name="pack",
        )(far(current), *nodes)
        got = swapped(packed, "sy")
        partial, row0, col0 = pl.pallas_call(
            near_kernel,
            in_specs=[WHOLE] * 3,
            out_specs=[WHOLE] * 3,
            out_shape=[KEPT, SPREAD, SPREAD],
            scratch_shapes=(COLUMNS, COLUMNS, PAIR, PAIR),
            compiler_params=PARAMS,
            cost_estimate=cost(20_000_000),
            name="near",
        )(packed, rows, cols)
        sent = pl.pallas_call(
            partner_kernel,
            in_specs=[WHOLE] * 4,
            out_specs=WHOLE,
            out_shape=KEPT,
            scratch_shapes=(COLUMNS, COLUMNS, PAIR, PAIR),
            compiler_params=PARAMS,
            name="partner",
        )(got, row0, col0, partial)
        made = pl.pallas_call(
            second_kernel,
            in_specs=[WHOLE] * 4 + [ANY] * 4,
            out_specs=[WHOLE] * 3,
            out_shape=[KEPT, MADE, MADE],
            scratch_shapes=node_buffers(None)
            + (COLUMNS, COLUMNS, SPREAD, SPREAD, ONE, ONE, pltpu.SemaphoreType.DMA((4,))),
            compiler_params=PARAMS,
            cost_estimate=cost(60_000_000),
            name="second",
        )(packed, got, row0, col0, *nodes)
        pieces = swapped(sent, "sx")
        sent, current = pl.pallas_call(
            middle_kernel,
            in_specs=[WHOLE] * 4,
            out_specs=[ANY, WHOLE],
            out_shape=[SENT, KEPT],
            scratch_shapes=(LEFT, STAGE, pltpu.SemaphoreType.DMA((FOREIGN,))),
            compiler_params=PARAMS,
            name="middle",
        )(pieces, *made)
        made = pl.pallas_call(
            between_kernel,
            in_specs=[WHOLE] + [ANY] * 4,
            out_specs=[WHOLE] * 3,
            out_shape=[
                KEPT,
                pltpu.VMEM((4 * BOXES, 2 * NODES, NODES), jnp.bfloat16),
                pltpu.VMEM((4 * BOXES, 2 * NODES, NODES), jnp.float8_e4m3fn),
            ],
            scratch_shapes=node_buffers(2) + TABLES + (ONE, ONE, LEFT, pltpu.SemaphoreType.DMA((4,))),
            compiler_params=PARAMS,
            cost_estimate=cost(60_000_000),
            name="between",
        )(current, *nodes)
        pieces = exchange(sent, 1)
        sent = pl.pallas_call(
            late_kernel,
            in_specs=[WHOLE] * 4,
            out_specs=WHOLE,
            out_shape=pltpu.VMEM((4,) + FIELD, jnp.float32),
            scratch_shapes=(LEFT,),
            compiler_params=PARAMS,
            name="late",
        )(pieces, *made)
        field = pl.pallas_call(
            final_kernel,
            in_specs=[WHOLE],
            out_specs=WHOLE,
            out_shape=jax.ShapeDtypeStruct(FIELD, jnp.float32),
            compiler_params=PARAMS,
            name="final",
        )(exchange(sent, 2))
        return field.reshape(2, BOXES, 1, RHS, NODES)

    in_specs = (
        P(None, "sx", "sy", None, None),
        P(None, None, "sx", "sy", None),
        P(None, None, None, None, "sx", "sy", None),
        P(),
        P(),
    )
    out_specs = P(None, "sx", "sy", None, None)
    return jax.shard_map(local, mesh=mesh, in_specs=in_specs, out_specs=out_specs, check_vma=False)
```

```python
import functools
import math

import jax
import jax.numpy as jnp
import numpy as np
from jax import lax
from jax.experimental import pallas as pl
from jax.experimental.pallas import tpu as pltpu
from jax.sharding import PartitionSpec as P

LEVELS = 3
CHEB = 16
NODES = CHEB * CHEB
RHS = 16
BOXES = 2
FOREIGN = 3
ITEMS = FOREIGN * BOXES
ROOT2 = math.sqrt(2.0)
SOURCE_LINE = 2 * BOXES * RHS
TARGET_LINE = SOURCE_LINE + 2 * BOXES
PACKED = 88
LOW_SCALE = 2.0**17


def half_turn_coefficients():
    nodes = 0.5 * np.cos((np.arange(64) + 0.5) * np.pi / 128)
    powers = np.stack([nodes, nodes**3, nodes**5], axis=1)
    wanted = 2.0**0.75 * np.sin(0.5 * np.pi * nodes)
    return [float(c) for c in np.linalg.lstsq(powers, wanted, rcond=None)[0]]


C0, C1, C2 = half_turn_coefficients()


def group_members(mesh, bit):
    n_rows, n_cols = mesh.shape["sx"], mesh.shape["sy"]
    step = 1 << bit
    groups = []
    for row in range(n_rows):
        for col in range(n_cols):
            if not row & step and not col & step:
                groups.append(
                    [(row + a) * n_cols + col + c for a in (0, step) for c in (0, step)]
                )
    return groups


def swapped(block, axis):
    count = lax.axis_size(axis)
    return lax.ppermute(block, axis, [(i, i ^ 1) for i in range(count)])


def fetch(pairs, sems):
    copies = [pltpu.make_async_copy(a, b, sems.at[i]) for i, (a, b) in enumerate(pairs)]
    for copy in copies:
        copy.start()
    return copies


def own_position(level):
    step = 1 << level
    row = lax.axis_index("sx") // step % 2
    col = lax.axis_index("sy") // step % 2
    return 2 * row + col


def spread_matrices(rows, cols, row_ref, col_ref):
    lane = lax.broadcasted_iota(jnp.int32, (CHEB, NODES), 1)
    node = lax.broadcasted_iota(jnp.int32, (CHEB, NODES), 0)
    outer = (lane // CHEB == node).astype(jnp.float32)
    inner = (lane % CHEB == node).astype(jnp.float32)
    spread = functools.partial(
        lax.dot_general,
        dimension_numbers=(((0,), (0,)), ((), ())),
        precision=lax.Precision.HIGHEST,
        preferred_element_type=jnp.float32,
    )
    for bit in range(2):
        row_ref[bit] = spread(rows[bit], outer)
        col_ref[bit] = spread(cols[bit], inner)


def normalize(matrices, normal, level):
    for bit in range(2):
        values = matrices[bit]
        top = jnp.max(jnp.abs(values), axis=(0, 1), keepdims=True)
        safe = jnp.where(top > 0.0, top, 1.0)
        normal[bit] = values / safe
        level[pl.ds(bit, 1), :] = jnp.broadcast_to(safe, (1, 128))


def spread_sources(source, a_ref, b_ref):
    lines = []
    for box in range(BOXES):
        freq = source(0, box)
        slow = source(1, box)
        near = 16.0 * freq * freq
        lines += [near, near * slow * slow]
    columns = jnp.concatenate(lines + lines, axis=0).T
    for box in range(BOXES):
        a_ref[box] = jnp.broadcast_to(columns[:, 2 * box : 2 * box + 1], (NODES, 128))
        b_ref[box] = jnp.broadcast_to(columns[:, 2 * box + 1 : 2 * box + 2], (NODES, 128))


def prepare(sources, rows, cols, tables):
    a_ref, b_ref, row_ref, col_ref = tables
    spread_matrices(rows, cols, row_ref, col_ref)
    spread_sources(lambda kind, box: sources[kind, box], a_ref, b_ref)


def line_of(targets):
    return lambda kind, row_bit, col_bit, box: targets[kind, row_bit, col_bit, box]


def weigh(position, box, target, tables, high, low):
    a_ref, b_ref, row_ref, col_ref = tables
    row_bit, col_bit = position // 2, position % 2
    tau = target(0, row_bit, col_bit, box)
    off = target(1, row_bit, col_bit, box)
    tau2, off2 = tau * tau, off * off
    inner = col_ref[col_bit]
    for step in range(CHEB):
        down = pl.ds(step * CHEB, CHEB)
        along = pl.ds(NODES + step * CHEB, CHEB)
        near = a_ref[box, down, :]
        far = b_ref[box, down, :]
        near = jnp.concatenate([near, near], axis=1)
        far = jnp.concatenate([far, far], axis=1)
        kron = row_ref[row_bit, pl.ds(step, 1), :] * inner
        z = near * tau2 + far * off2
        turns = z * lax.rsqrt(z)
        rest = turns - jnp.round(turns)
        y = rest * rest
        half = rest * (C0 + y * (C1 + y * C2))
        q = half * half
        cosine = ROOT2 - q
        v = 2.0 * ROOT2 - q
        sine = half * (v * lax.rsqrt(v))
        part = kron * sine
        real = kron - part * sine
        imag = part * cosine
        for where, value in ((down, real), (along, imag)):
            top = value.astype(jnp.bfloat16)
            high[where, :] = top
            rest_of = value - top.astype(jnp.float32)
            if low.dtype != jnp.bfloat16:
                rest_of = rest_of * LOW_SCALE
            low[where, :] = rest_of.astype(low.dtype)


def stacked(values):
    def turned(x):
        return jnp.concatenate([-x[RHS:], x[:RHS]], axis=0)

    top = values.astype(jnp.bfloat16)
    rest = (values - top.astype(jnp.float32)).astype(jnp.bfloat16)
    left = jnp.concatenate([top, rest], axis=0)
    right = jnp.concatenate([turned(top), turned(rest)], axis=0)
    return jnp.concatenate([left, right], axis=1)


def stack_boxes(real, imag, left):
    for box in range(BOXES):
        left[box] = stacked(jnp.concatenate([real[box], imag[box]], axis=0))


def product(left, high, low):
    main = jnp.dot(left, high, preferred_element_type=jnp.float32)
    scaled = low.dtype != jnp.bfloat16
    small = jnp.dot(
        left[: 2 * RHS], low, preferred_element_type=jnp.float32
    )
    if scaled:
        small = small * (1.0 / LOW_SCALE)
    return main[: 2 * RHS] + main[2 * RHS :] + small


def put(out, index, box, total):
    out[index, 0, box] = total[:RHS]
    out[index, 1, box] = total[RHS:]


def packed_source(packed):
    return lambda kind, box: packed[pl.ds(SOURCE_LINE + 2 * kind + box, 1), :]


def packed_target(packed):
    def line(kind, row_bit, col_bit, box):
        place = ((kind * 2 + row_bit) * 2 + col_bit) * BOXES + box
        return packed[pl.ds(TARGET_LINE + place, 1), :]

    return line


def packed_values(packed, box):
    real = packed[box * RHS : (box + 1) * RHS, :]
    imag = packed[(BOXES + box) * RHS : (BOXES + box + 1) * RHS, :]
    return jnp.concatenate([real, imag], axis=0)


def pack_kernel(
    coeffs_hbm, sources_hbm, targets_hbm, rows_hbm, cols_hbm, packed, rows, cols,
    coeffs, sources, targets, sems,
):
    copies = fetch(
        [
            (coeffs_hbm, coeffs),
            (sources_hbm.at[0], sources),
            (targets_hbm.at[0], targets),
            (rows_hbm.at[0], rows),
            (cols_hbm.at[0], cols),
        ],
        sems,
    )
    for copy in copies:
        copy.wait()
    for part in range(2):
        for box in range(BOXES):
            packed[pl.ds((part * BOXES + box) * RHS, RHS), :] = coeffs[part, box]
    lines = [sources[kind, box] for kind in range(2) for box in range(BOXES)]
    for kind in range(2):
        for place in range(4 * BOXES):
            lines.append(targets[kind, place // 4, place // 2 % 2, place % 2])
    lines += [lines[-1]] * (PACKED - SOURCE_LINE - len(lines))
    packed[pl.ds(SOURCE_LINE, PACKED - SOURCE_LINE), :] = jnp.concatenate(lines, axis=0)


def pair_of_boxes(packed, position, tables, high, low):
    target = packed_target(packed)
    for box in range(BOXES):
        weigh(position, box, target, tables, high.at[box], low.at[box])
    return [
        product(stacked(packed_values(packed, box)), high[box], low[box]) for box in range(BOXES)
    ]


def near_kernel(packed, rows, cols, partial, row_ref, col_ref, a_ref, b_ref, high, low):
    spread_matrices(rows, cols, row_ref, col_ref)
    spread_sources(packed_source(packed), a_ref, b_ref)
    tables = (a_ref, b_ref, row_ref, col_ref)
    both = pair_of_boxes(packed, own_position(0) ^ 2, tables, high, low)
    for box in range(BOXES):
        partial[0, box] = both[box][:RHS]
        partial[1, box] = both[box][RHS:]


def partner_kernel(packed, row_ref, col_ref, partial, sent, a_ref, b_ref, high, low):
    spread_sources(packed_source(packed), a_ref, b_ref)
    tables = (a_ref, b_ref, row_ref, col_ref)
    both = pair_of_boxes(packed, own_position(0) ^ 2, tables, high, low)
    for box in range(BOXES):
        sent[0, box] = partial[0, box] + both[box][:RHS]
        sent[1, box] = partial[1, box] + both[box][RHS:]


def make_weights(level, first, targets, tables, high, low):
    there = own_position(level)

    def make(item, carry):
        weigh(
            there ^ (item // 2 + first),
            item % 2,
            line_of(targets),
            tables,
            high.at[item],
            low.at[item],
        )
        return carry

    lax.fori_loop(0, (4 - first) * BOXES, make, 0)


def second_kernel(
    packed, got, row0_ref, col0_ref, sources_hbm, targets_hbm, rows_hbm, cols_hbm, own, high, low,
    sources, targets, rows, cols, *rest,
):
    a_ref, b_ref, row_ref, col_ref, own_high, own_low, sems = rest
    nodes = fetch(
        [
            (sources_hbm.at[1], sources),
            (rows_hbm.at[1], rows),
            (cols_hbm.at[1], cols),
            (targets_hbm.at[1], targets),
        ],
        sems,
    )
    me = own_position(0)
    tables = (a_ref, b_ref, row0_ref, col0_ref)
    for index, lines in enumerate((packed, got)):
        spread_sources(packed_source(lines), a_ref, b_ref)

        def mine(box, carry):
            weigh(me, box, packed_target(lines), tables, own_high, own_low)
            start = pl.multiple_of(box * RHS, RHS)
            real = lines[pl.ds(start, RHS), :]
            imag = lines[pl.ds(start + BOXES * RHS, RHS), :]
            left = stacked(jnp.concatenate([real, imag], axis=0))
            total = product(left, own_high[...], own_low[...])
            if index:
                own[0, box] += total[:RHS]
                own[1, box] += total[RHS:]
            else:
                own[0, box] = total[:RHS]
                own[1, box] = total[RHS:]
            return carry

        lax.fori_loop(0, BOXES, mine, 0)
    for copy in nodes:
        copy.wait()
    tables = (a_ref, b_ref, row_ref, col_ref)
    prepare(sources, rows, cols, tables)
    make_weights(1, 1, targets, tables, high, low)


def between_kernel(
    values, sources_hbm, targets_hbm, rows_hbm, cols_hbm, own, high, low, row_size, col_size,
    sources, targets, rows, cols, *rest,
):
    *tables, own_high, own_low, left, row_normal, col_normal, sems = rest
    here = pl.ds(1, 2)
    nodes = fetch(
        [
            (sources_hbm.at[here], sources),
            (rows_hbm.at[here], rows),
            (cols_hbm.at[here], cols),
            (targets_hbm.at[here], targets),
        ],
        sems,
    )
    stack_boxes(values[0], values[1], left)
    for copy in nodes:
        copy.wait()
    prepare(sources.at[0], rows.at[0], cols.at[0], tables)
    me = own_position(1)

    def mine(box, carry):
        weigh(me, box, line_of(targets.at[0]), tables, own_high, own_low)
        total = product(left[box], own_high[...], own_low[...])
        own[0, box] = total[:RHS]
        own[1, box] = total[RHS:]
        return carry

    lax.fori_loop(0, BOXES, mine, 0)
    normalize(rows.at[1], row_normal, row_size)
    normalize(cols.at[1], col_normal, col_size)
    prepare(sources.at[1], row_normal, col_normal, tables)
    make_weights(2, 0, targets.at[1], tables, high, low)


def middle_kernel(piece, own, high, low, out_hbm, current, left, stage, sems):
    values = own[...] + piece[...]
    current[...] = values
    stack_boxes(values[0], values[1], left)
    me = own_position(1)
    sent = []
    for x in range(FOREIGN):
        for box in range(BOXES):
            item = 2 * x + box
            put(stage, x, box, product(left[box], high[item], low[item]))
        copy = pltpu.make_async_copy(stage.at[x], out_hbm.at[me ^ (x + 1)], sems.at[x])
        copy.start()
        sent.append(copy)
    for copy in sent:
        copy.wait()


def late_kernel(pieces, own, high, low, row_size, col_size, out, left):
    me = own_position(1)
    values = (own[...] + pieces[me ^ 1]) + (pieces[me ^ 2] + pieces[me ^ 3])
    stack_boxes(values[0], values[1], left)
    there = own_position(2)
    for x in range(4):
        place = there ^ x
        size = row_size[pl.ds(place // 2, 1), :] * col_size[pl.ds(place % 2, 1), :]
        size = jnp.concatenate([size, size], axis=1)
        for box in range(BOXES):
            item = 2 * x + box
            put(out, place, box, product(left[box], high[item], low[item]) * size)


def final_kernel(pieces, out):
    out[...] = (pieces[0] + pieces[1]) + (pieces[2] + pieces[3])


def node_buffers(count):
    lead = () if count is None else (count,)
    return (
        pltpu.VMEM(lead + (2, BOXES, 1, NODES), jnp.float32),
        pltpu.VMEM(lead + (2, 2, 2, BOXES, 1, NODES), jnp.float32),
        pltpu.VMEM(lead + (2, CHEB, CHEB), jnp.float32),
        pltpu.VMEM(lead + (2, CHEB, CHEB), jnp.float32),
    )


TABLES = (
    pltpu.VMEM((BOXES, NODES, 128), jnp.float32),
    pltpu.VMEM((BOXES, NODES, 128), jnp.float32),
    pltpu.VMEM((2, CHEB, NODES), jnp.float32),
    pltpu.VMEM((2, CHEB, NODES), jnp.float32),
)
FIELD = (2, BOXES, RHS, NODES)
LEFT = pltpu.VMEM((BOXES, 4 * RHS, 2 * NODES), jnp.bfloat16)
STAGE = pltpu.VMEM((FOREIGN,) + FIELD, jnp.float32)
ANY = pl.BlockSpec(memory_space=pltpu.HBM)
WHOLE = pl.BlockSpec(memory_space=pltpu.VMEM)
PARAMS = pltpu.CompilerParams(vmem_limit_bytes=12 * 1024 * 1024)


SENT = pltpu.HBM((4,) + FIELD, jnp.float32)
KEPT = pltpu.VMEM(FIELD, jnp.float32)
SPREAD = pltpu.VMEM((2, CHEB, NODES), jnp.float32)
SMALL = pltpu.VMEM((2, CHEB, CHEB), jnp.float32)
ONE = pltpu.VMEM((2 * NODES, NODES), jnp.bfloat16)
PAIR = pltpu.VMEM((BOXES, 2 * NODES, NODES), jnp.bfloat16)
COLUMNS = pltpu.VMEM((BOXES, NODES, 128), jnp.float32)
MADE = pltpu.VMEM((ITEMS, 2 * NODES, NODES), jnp.bfloat16)


def far(x):
    return pltpu.with_memory_space_constraint(x, pltpu.HBM)


def cost(flops):
    return pl.CostEstimate(flops=flops, bytes_accessed=100_000, transcendentals=0)


def solution(mesh):
    groups = [group_members(mesh, bit) for bit in range(LEVELS)]

    def exchange(sent, level):
        return lax.all_to_all(
            sent, ("sx", "sy"), 0, 0, axis_index_groups=groups[level], tiled=True
        )

    def local(coeffs, source_nodes, target_nodes, interp_rows, interp_cols):
        current = coeffs.reshape(FIELD)
        nodes = (
            far(source_nodes.reshape(LEVELS, 2, BOXES, 1, NODES)),
            far(target_nodes.reshape(LEVELS, 2, 2, 2, BOXES, 1, NODES)),
            far(interp_rows),
            far(interp_cols),
        )
        packed, rows, cols = pl.pallas_call(
            pack_kernel,
            in_specs=[ANY] * 5,
            out_specs=[WHOLE] * 3,
            out_shape=[pltpu.VMEM((PACKED, NODES), jnp.float32), SMALL, SMALL],
            scratch_shapes=(KEPT,) + node_buffers(None)[:2] + (pltpu.SemaphoreType.DMA((5,)),),
            compiler_params=PARAMS,
            name="pack",
        )(far(current), *nodes)
        got = swapped(packed, "sy")
        partial, row0, col0 = pl.pallas_call(
            near_kernel,
            in_specs=[WHOLE] * 3,
            out_specs=[WHOLE] * 3,
            out_shape=[KEPT, SPREAD, SPREAD],
            scratch_shapes=(COLUMNS, COLUMNS, PAIR, PAIR),
            compiler_params=PARAMS,
            cost_estimate=cost(20_000_000),
            name="near",
        )(packed, rows, cols)
        sent = pl.pallas_call(
            partner_kernel,
            in_specs=[WHOLE] * 4,
            out_specs=WHOLE,
            out_shape=KEPT,
            scratch_shapes=(COLUMNS, COLUMNS, PAIR, PAIR),
            compiler_params=PARAMS,
            name="partner",
        )(got, row0, col0, partial)
        made = pl.pallas_call(
            second_kernel,
            in_specs=[WHOLE] * 4 + [ANY] * 4,
            out_specs=[WHOLE] * 3,
            out_shape=[KEPT, MADE, MADE],
            scratch_shapes=node_buffers(None)
            + (COLUMNS, COLUMNS, SPREAD, SPREAD, ONE, ONE, pltpu.SemaphoreType.DMA((4,))),
            compiler_params=PARAMS,
            cost_estimate=cost(60_000_000),
            name="second",
        )(packed, got, row0, col0, *nodes)
        pieces = swapped(sent, "sx")
        sent, current = pl.pallas_call(
            middle_kernel,
            in_specs=[WHOLE] * 4,
            out_specs=[ANY, WHOLE],
            out_shape=[SENT, KEPT],
            scratch_shapes=(LEFT, STAGE, pltpu.SemaphoreType.DMA((FOREIGN,))),
            compiler_params=PARAMS,
            name="middle",
        )(pieces, *made)
        made = pl.pallas_call(
            between_kernel,
            in_specs=[WHOLE] + [ANY] * 4,
            out_specs=[WHOLE] * 5,
            out_shape=[
                KEPT,
                pltpu.VMEM((4 * BOXES, 2 * NODES, NODES), jnp.bfloat16),
                pltpu.VMEM((4 * BOXES, 2 * NODES, NODES), jnp.float8_e4m3fn),
                pltpu.VMEM((2, 128), jnp.float32),
                pltpu.VMEM((2, 128), jnp.float32),
            ],
            scratch_shapes=node_buffers(2)
            + TABLES
            + (ONE, ONE, LEFT, SMALL, SMALL, pltpu.SemaphoreType.DMA((4,))),
            compiler_params=PARAMS,
            cost_estimate=cost(60_000_000),
            name="between",
        )(current, *nodes)
        pieces = exchange(sent, 1)
        sent = pl.pallas_call(
            late_kernel,
            in_specs=[WHOLE] * 6,
            out_specs=WHOLE,
            out_shape=pltpu.VMEM((4,) + FIELD, jnp.float32),
            scratch_shapes=(LEFT,),
            compiler_params=PARAMS,
            name="late",
        )(pieces, *made)
        field = pl.pallas_call(
            final_kernel,
            in_specs=[WHOLE],
            out_specs=WHOLE,
            out_shape=jax.ShapeDtypeStruct(FIELD, jnp.float32),
            compiler_params=PARAMS,
            name="final",
        )(exchange(sent, 2))
        return field.reshape(2, BOXES, 1, RHS, NODES)

    in_specs = (
        P(None, "sx", "sy", None, None),
        P(None, None, "sx", "sy", None),
        P(None, None, None, None, "sx", "sy", None),
        P(),
        P(),
    )
    out_specs = P(None, "sx", "sy", None, None)
    return jax.shard_map(local, mesh=mesh, in_specs=in_specs, out_specs=out_specs, check_vma=False)
```

```python
import functools
import math

import jax
import jax.numpy as jnp
import numpy as np
from jax import lax
from jax.experimental import pallas as pl
from jax.experimental.pallas import tpu as pltpu
from jax.sharding import PartitionSpec as P

LEVELS = 3
CHEB = 16
NODES = CHEB * CHEB
RHS = 16
BOXES = 2
FOREIGN = 3
ITEMS = FOREIGN * BOXES
ROOT2 = math.sqrt(2.0)
SOURCE_LINE = 2 * BOXES * RHS
TARGET_LINE = SOURCE_LINE + 2 * BOXES
PACKED = 88
LOW_SCALE = 2.0**17


def half_turn_coefficients():
    nodes = 0.5 * np.cos((np.arange(64) + 0.5) * np.pi / 128)
    powers = np.stack([nodes, nodes**3, nodes**5], axis=1)
    wanted = 2.0**0.75 * np.sin(0.5 * np.pi * nodes)
    return [float(c) for c in np.linalg.lstsq(powers, wanted, rcond=None)[0]]


C0, C1, C2 = half_turn_coefficients()


def group_members(mesh, bit):
    n_rows, n_cols = mesh.shape["sx"], mesh.shape["sy"]
    step = 1 << bit
    groups = []
    for row in range(n_rows):
        for col in range(n_cols):
            if not row & step and not col & step:
                groups.append(
                    [(row + a) * n_cols + col + c for a in (0, step) for c in (0, step)]
                )
    return groups


def swapped(block, axis):
    count = lax.axis_size(axis)
    return lax.ppermute(block, axis, [(i, i ^ 1) for i in range(count)])


def fetch(pairs, sems):
    copies = [pltpu.make_async_copy(a, b, sems.at[i]) for i, (a, b) in enumerate(pairs)]
    for copy in copies:
        copy.start()
    return copies


def own_position(level):
    step = 1 << level
    row = lax.axis_index("sx") // step % 2
    col = lax.axis_index("sy") // step % 2
    return 2 * row + col


def spread_matrices(rows, cols, row_ref, col_ref):
    lane = lax.broadcasted_iota(jnp.int32, (CHEB, NODES), 1)
    node = lax.broadcasted_iota(jnp.int32, (CHEB, NODES), 0)
    outer = (lane // CHEB == node).astype(jnp.float32)
    inner = (lane % CHEB == node).astype(jnp.float32)
    spread = functools.partial(
        lax.dot_general,
        dimension_numbers=(((0,), (0,)), ((), ())),
        precision=lax.Precision.HIGHEST,
        preferred_element_type=jnp.float32,
    )
    for bit in range(2):
        row_ref[bit] = spread(rows[bit], outer)
        col_ref[bit] = spread(cols[bit], inner)


def normalize(matrices, normal, level):
    for bit in range(2):
        values = matrices[bit]
        top = jnp.max(jnp.abs(values), axis=(0, 1), keepdims=True)
        safe = jnp.where(top > 0.0, top, 1.0)
        normal[bit] = values / safe
        level[pl.ds(bit, 1), :] = jnp.broadcast_to(safe, (1, 128))


def spread_sources(source, a_ref, b_ref):
    lines = []
    for box in range(BOXES):
        freq = source(0, box)
        slow = source(1, box)
        near = 16.0 * freq * freq
        lines += [near, near * slow * slow]
    columns = jnp.concatenate(lines + lines, axis=0).T
    for box in range(BOXES):
        a_ref[box] = jnp.broadcast_to(columns[:, 2 * box : 2 * box + 1], (NODES, 128))
        b_ref[box] = jnp.broadcast_to(columns[:, 2 * box + 1 : 2 * box + 2], (NODES, 128))


def prepare(sources, rows, cols, tables):
    a_ref, b_ref, row_ref, col_ref = tables
    spread_matrices(rows, cols, row_ref, col_ref)
    spread_sources(lambda kind, box: sources[kind, box], a_ref, b_ref)


def line_of(targets):
    return lambda kind, row_bit, col_bit, box: targets[kind, row_bit, col_bit, box]


def weigh(position, box, target, tables, high, low):
    a_ref, b_ref, row_ref, col_ref = tables
    row_bit, col_bit = position // 2, position % 2
    tau = target(0, row_bit, col_bit, box)
    off = target(1, row_bit, col_bit, box)
    tau2, off2 = tau * tau, off * off
    inner = col_ref[col_bit]
    for step in range(CHEB):
        down = pl.ds(step * CHEB, CHEB)
        along = pl.ds(NODES + step * CHEB, CHEB)
        near = a_ref[box, down, :]
        far = b_ref[box, down, :]
        near = jnp.concatenate([near, near], axis=1)
        far = jnp.concatenate([far, far], axis=1)
        kron = row_ref[row_bit, pl.ds(step, 1), :] * inner
        z = near * tau2 + far * off2
        turns = z * lax.rsqrt(z)
        rest = turns - jnp.round(turns)
        y = rest * rest
        half = rest * (C0 + y * (C1 + y * C2))
        q = half * half
        cosine = ROOT2 - q
        v = 2.0 * ROOT2 - q
        sine = half * (v * lax.rsqrt(v))
        part = kron * sine
        real = kron - part * sine
        imag = part * cosine
        for where, value in ((down, real), (along, imag)):
            top = value.astype(jnp.bfloat16)
            high[where, :] = top
            rest_of = value - top.astype(jnp.float32)
            if low.dtype != jnp.bfloat16:
                rest_of = rest_of * LOW_SCALE
            low[where, :] = rest_of.astype(low.dtype)


def stacked(values):
    def turned(x):
        return jnp.concatenate([-x[RHS:], x[:RHS]], axis=0)

    top = values.astype(jnp.bfloat16)
    rest = (values - top.astype(jnp.float32)).astype(jnp.bfloat16)
    left = jnp.concatenate([top, rest], axis=0)
    right = jnp.concatenate([turned(top), turned(rest)], axis=0)
    return jnp.concatenate([left, right], axis=1)


def stack_boxes(real, imag, left):
    for box in range(BOXES):
        left[box] = stacked(jnp.concatenate([real[box], imag[box]], axis=0))


def product(left, high, low):
    main = jnp.dot(left, high, preferred_element_type=jnp.float32)
    scaled = low.dtype != jnp.bfloat16
    small = jnp.dot(
        left[: 2 * RHS], low, preferred_element_type=jnp.float32
    )
    if scaled:
        small = small * (1.0 / LOW_SCALE)
    return main[: 2 * RHS] + main[2 * RHS :] + small


def put(out, index, box, total):
    out[index, 0, box] = total[:RHS]
    out[index, 1, box] = total[RHS:]


def packed_source(packed):
    return lambda kind, box: packed[pl.ds(SOURCE_LINE + 2 * kind + box, 1), :]


def packed_target(packed):
    def line(kind, row_bit, col_bit, box):
        place = ((kind * 2 + row_bit) * 2 + col_bit) * BOXES + box
        return packed[pl.ds(TARGET_LINE + place, 1), :]

    return line


def packed_values(packed, box):
    real = packed[box * RHS : (box + 1) * RHS, :]
    imag = packed[(BOXES + box) * RHS : (BOXES + box + 1) * RHS, :]
    return jnp.concatenate([real, imag], axis=0)


def pack_kernel(
    coeffs_hbm, sources_hbm, targets_hbm, rows_hbm, cols_hbm, packed, rows, cols,
    coeffs, sources, targets, sems,
):
    copies = fetch(
        [
            (coeffs_hbm, coeffs),
            (sources_hbm.at[0], sources),
            (targets_hbm.at[0], targets),
            (rows_hbm.at[0], rows),
            (cols_hbm.at[0], cols),
        ],
        sems,
    )
    for copy in copies:
        copy.wait()
    for part in range(2):
        for box in range(BOXES):
            packed[pl.ds((part * BOXES + box) * RHS, RHS), :] = coeffs[part, box]
    lines = [sources[kind, box] for kind in range(2) for box in range(BOXES)]
    for kind in range(2):
        for place in range(4 * BOXES):
            lines.append(targets[kind, place // 4, place // 2 % 2, place % 2])
    lines += [lines[-1]] * (PACKED - SOURCE_LINE - len(lines))
    packed[pl.ds(SOURCE_LINE, PACKED - SOURCE_LINE), :] = jnp.concatenate(lines, axis=0)


def pair_of_boxes(packed, position, tables, high, low):
    target = packed_target(packed)
    for box in range(BOXES):
        weigh(position, box, target, tables, high.at[box], low.at[box])
    return [
        product(stacked(packed_values(packed, box)), high[box], low[box]) for box in range(BOXES)
    ]


def near_kernel(packed, rows, cols, partial, row_ref, col_ref, a_ref, b_ref, high, low):
    spread_matrices(rows, cols, row_ref, col_ref)
    spread_sources(packed_source(packed), a_ref, b_ref)
    tables = (a_ref, b_ref, row_ref, col_ref)
    both = pair_of_boxes(packed, own_position(0) ^ 2, tables, high, low)
    for box in range(BOXES):
        partial[0, box] = both[box][:RHS]
        partial[1, box] = both[box][RHS:]


def partner_kernel(packed, row_ref, col_ref, partial, sent, a_ref, b_ref, high, low):
    spread_sources(packed_source(packed), a_ref, b_ref)
    tables = (a_ref, b_ref, row_ref, col_ref)
    both = pair_of_boxes(packed, own_position(0) ^ 2, tables, high, low)
    for box in range(BOXES):
        sent[0, box] = partial[0, box] + both[box][:RHS]
        sent[1, box] = partial[1, box] + both[box][RHS:]


def make_weights(level, first, targets, tables, high, low):
    there = own_position(level)

    def make(item, carry):
        weigh(
            there ^ (item // 2 + first),
            item % 2,
            line_of(targets),
            tables,
            high.at[item],
            low.at[item],
        )
        return carry

    lax.fori_loop(0, (4 - first) * BOXES, make, 0)


def second_kernel(
    packed, got, row0_ref, col0_ref, a_near, b_near, a_got, b_got,
    sources_hbm, targets_hbm, rows_hbm, cols_hbm,
    own, high, low,
    sources, targets, rows, cols, a_ref, b_ref, row_ref, col_ref, own_high, own_low, sems,
):
    nodes = fetch(
        [
            (sources_hbm.at[1], sources),
            (rows_hbm.at[1], rows),
            (cols_hbm.at[1], cols),
            (targets_hbm.at[1], targets),
        ],
        sems,
    )
    me = own_position(0)
    for index, (lines, a0, b0) in enumerate(((packed, a_near, b_near), (got, a_got, b_got))):

        def mine(box, carry):
            weigh(me, box, packed_target(lines), (a0, b0, row0_ref, col0_ref), own_high, own_low)
            start = pl.multiple_of(box * RHS, RHS)
            real = lines[pl.ds(start, RHS), :]
            imag = lines[pl.ds(start + BOXES * RHS, RHS), :]
            left = stacked(jnp.concatenate([real, imag], axis=0))
            total = product(left, own_high[...], own_low[...])
            if index:
                own[0, box] += total[:RHS]
                own[1, box] += total[RHS:]
            else:
                own[0, box] = total[:RHS]
                own[1, box] = total[RHS:]
            return carry

        lax.fori_loop(0, BOXES, mine, 0)
    for copy in nodes:
        copy.wait()
    tables = (a_ref, b_ref, row_ref, col_ref)
    prepare(sources, rows, cols, tables)
    make_weights(1, 1, targets, tables, high, low)


def between_kernel(
    values, sources_hbm, targets_hbm, rows_hbm, cols_hbm, own, high, low, row_size, col_size,
    sources, targets, rows, cols, *rest,
):
    *tables, own_high, own_low, left, row_normal, col_normal, sems = rest
    here = pl.ds(1, 2)
    nodes = fetch(
        [
            (sources_hbm.at[here], sources),
            (rows_hbm.at[here], rows),
            (cols_hbm.at[here], cols),
            (targets_hbm.at[here], targets),
        ],
        sems,
    )
    stack_boxes(values[0], values[1], left)
    for copy in nodes:
        copy.wait()
    prepare(sources.at[0], rows.at[0], cols.at[0], tables)
    me = own_position(1)

    def mine(box, carry):
        weigh(me, box, line_of(targets.at[0]), tables, own_high, own_low)
        total = product(left[box], own_high[...], own_low[...])
        own[0, box] = total[:RHS]
        own[1, box] = total[RHS:]
        return carry

    lax.fori_loop(0, BOXES, mine, 0)
    normalize(rows.at[1], row_normal, row_size)
    normalize(cols.at[1], col_normal, col_size)
    prepare(sources.at[1], row_normal, col_normal, tables)
    make_weights(2, 0, targets.at[1], tables, high, low)


def middle_kernel(piece, own, high, low, out_hbm, current, left, stage, sems):
    values = own[...] + piece[...]
    current[...] = values
    stack_boxes(values[0], values[1], left)
    me = own_position(1)
    sent = []
    for x in range(FOREIGN):
        for box in range(BOXES):
            item = 2 * x + box
            put(stage, x, box, product(left[box], high[item], low[item]))
        copy = pltpu.make_async_copy(stage.at[x], out_hbm.at[me ^ (x + 1)], sems.at[x])
        copy.start()
        sent.append(copy)
    for copy in sent:
        copy.wait()


def late_kernel(pieces, own, high, low, row_size, col_size, out, left):
    me = own_position(1)
    values = (own[...] + pieces[me ^ 1]) + (pieces[me ^ 2] + pieces[me ^ 3])
    stack_boxes(values[0], values[1], left)
    there = own_position(2)
    for x in range(4):
        place = there ^ x
        size = row_size[pl.ds(place // 2, 1), :] * col_size[pl.ds(place % 2, 1), :]
        size = jnp.concatenate([size, size], axis=1)
        for box in range(BOXES):
            item = 2 * x + box
            put(out, place, box, product(left[box], high[item], low[item]) * size)


def final_kernel(pieces, out):
    out[...] = (pieces[0] + pieces[1]) + (pieces[2] + pieces[3])


def node_buffers(count):
    lead = () if count is None else (count,)
    return (
        pltpu.VMEM(lead + (2, BOXES, 1, NODES), jnp.float32),
        pltpu.VMEM(lead + (2, 2, 2, BOXES, 1, NODES), jnp.float32),
        pltpu.VMEM(lead + (2, CHEB, CHEB), jnp.float32),
        pltpu.VMEM(lead + (2, CHEB, CHEB), jnp.float32),
    )


TABLES = (
    pltpu.VMEM((BOXES, NODES, 128), jnp.float32),
    pltpu.VMEM((BOXES, NODES, 128), jnp.float32),
    pltpu.VMEM((2, CHEB, NODES), jnp.float32),
    pltpu.VMEM((2, CHEB, NODES), jnp.float32),
)
FIELD = (2, BOXES, RHS, NODES)
LEFT = pltpu.VMEM((BOXES, 4 * RHS, 2 * NODES), jnp.bfloat16)
STAGE = pltpu.VMEM((FOREIGN,) + FIELD, jnp.float32)
ANY = pl.BlockSpec(memory_space=pltpu.HBM)
WHOLE = pl.BlockSpec(memory_space=pltpu.VMEM)
PARAMS = pltpu.CompilerParams(vmem_limit_bytes=12 * 1024 * 1024)


SENT = pltpu.HBM((4,) + FIELD, jnp.float32)
KEPT = pltpu.VMEM(FIELD, jnp.float32)
SPREAD = pltpu.VMEM((2, CHEB, NODES), jnp.float32)
SMALL = pltpu.VMEM((2, CHEB, CHEB), jnp.float32)
ONE = pltpu.VMEM((2 * NODES, NODES), jnp.bfloat16)
PAIR = pltpu.VMEM((BOXES, 2 * NODES, NODES), jnp.bfloat16)
COLUMNS = pltpu.VMEM((BOXES, NODES, 128), jnp.float32)
MADE = pltpu.VMEM((ITEMS, 2 * NODES, NODES), jnp.bfloat16)


def far(x):
    return pltpu.with_memory_space_constraint(x, pltpu.HBM)


def cost(flops):
    return pl.CostEstimate(flops=flops, bytes_accessed=100_000, transcendentals=0)


def solution(mesh):
    groups = [group_members(mesh, bit) for bit in range(LEVELS)]

    def exchange(sent, level):
        return lax.all_to_all(
            sent, ("sx", "sy"), 0, 0, axis_index_groups=groups[level], tiled=True
        )

    def local(coeffs, source_nodes, target_nodes, interp_rows, interp_cols):
        current = coeffs.reshape(FIELD)
        nodes = (
            far(source_nodes.reshape(LEVELS, 2, BOXES, 1, NODES)),
            far(target_nodes.reshape(LEVELS, 2, 2, 2, BOXES, 1, NODES)),
            far(interp_rows),
            far(interp_cols),
        )
        packed, rows, cols = pl.pallas_call(
            pack_kernel,
            in_specs=[ANY] * 5,
            out_specs=[WHOLE] * 3,
            out_shape=[pltpu.VMEM((PACKED, NODES), jnp.float32), SMALL, SMALL],
            scratch_shapes=(KEPT,) + node_buffers(None)[:2] + (pltpu.SemaphoreType.DMA((5,)),),
            compiler_params=PARAMS,
            name="pack",
        )(far(current), *nodes)
        got = swapped(packed, "sy")
        partial, row0, col0, a_near, b_near = pl.pallas_call(
            near_kernel,
            in_specs=[WHOLE] * 3,
            out_specs=[WHOLE] * 5,
            out_shape=[KEPT, SPREAD, SPREAD, COLUMNS, COLUMNS],
            scratch_shapes=(PAIR, PAIR),
            compiler_params=PARAMS,
            cost_estimate=cost(20_000_000),
            name="near",
        )(packed, rows, cols)
        sent, a_got, b_got = pl.pallas_call(
            partner_kernel,
            in_specs=[WHOLE] * 4,
            out_specs=[WHOLE] * 3,
            out_shape=[KEPT, COLUMNS, COLUMNS],
            scratch_shapes=(PAIR, PAIR),
            compiler_params=PARAMS,
            name="partner",
        )(got, row0, col0, partial)
        own, high, low = pl.pallas_call(
            second_kernel,
            in_specs=[WHOLE] * 8 + [ANY] * 4,
            out_specs=[WHOLE] * 3,
            out_shape=[KEPT, MADE, MADE],
            scratch_shapes=node_buffers(None)
            + TABLES
            + (ONE, ONE, pltpu.SemaphoreType.DMA((4,))),
            compiler_params=PARAMS,
            cost_estimate=cost(60_000_000),
            name="second",
        )(packed, got, row0, col0, a_near, b_near, a_got, b_got, *nodes)
        pieces = swapped(sent, "sx")
        sent, current = pl.pallas_call(
            middle_kernel,
            in_specs=[WHOLE] * 4,
            out_specs=[ANY, WHOLE],
            out_shape=[SENT, KEPT],
            scratch_shapes=(LEFT, STAGE, pltpu.SemaphoreType.DMA((FOREIGN,))),
            compiler_params=PARAMS,
            name="middle",
        )(pieces, own, high, low)
        made = pl.pallas_call(
            between_kernel,
            in_specs=[WHOLE] + [ANY] * 4,
            out_specs=[WHOLE] * 5,
            out_shape=[
                KEPT,
                pltpu.VMEM((4 * BOXES, 2 * NODES, NODES), jnp.bfloat16),
                pltpu.VMEM((4 * BOXES, 2 * NODES, NODES), jnp.float8_e4m3fn),
                pltpu.VMEM((2, 128), jnp.float32),
                pltpu.VMEM((2, 128), jnp.float32),
            ],
            scratch_shapes=node_buffers(2)
            + TABLES
            + (ONE, ONE, LEFT, SMALL, SMALL, pltpu.SemaphoreType.DMA((4,))),
            compiler_params=PARAMS,
            cost_estimate=cost(60_000_000),
            name="between",
        )(current, *nodes)
        pieces = exchange(sent, 1)
        sent = pl.pallas_call(
            late_kernel,
            in_specs=[WHOLE] * 6,
            out_specs=WHOLE,
            out_shape=pltpu.VMEM((4,) + FIELD, jnp.float32),
            scratch_shapes=(LEFT,),
            compiler_params=PARAMS,
            name="late",
        )(pieces, *made)
        field = pl.pallas_call(
            final_kernel,
            in_specs=[WHOLE],
            out_specs=WHOLE,
            out_shape=jax.ShapeDtypeStruct(FIELD, jnp.float32),
            compiler_params=PARAMS,
            name="final",
        )(exchange(sent, 2))
        return field.reshape(2, BOXES, 1, RHS, NODES)

    in_specs = (
        P(None, "sx", "sy", None, None),
        P(None, None, "sx", "sy", None),
        P(None, None, None, None, "sx", "sy", None),
        P(),
        P(),
    )
    out_specs = P(None, "sx", "sy", None, None)
    return jax.shard_map(local, mesh=mesh, in_specs=in_specs, out_specs=out_specs, check_vma=False)
```

```python
import functools
import math

import jax
import jax.numpy as jnp
import numpy as np
from jax import lax
from jax.experimental import pallas as pl
from jax.experimental.pallas import tpu as pltpu
from jax.sharding import PartitionSpec as P

LEVELS = 3
CHEB = 16
NODES = CHEB * CHEB
RHS = 16
BOXES = 2
FOREIGN = 3
ITEMS = FOREIGN * BOXES
ROOT2 = math.sqrt(2.0)
SOURCE_LINE = 2 * BOXES * RHS
TARGET_LINE = SOURCE_LINE + 2 * BOXES
PACKED = 88
LOW_SCALE = 2.0**17


def half_turn_coefficients():
    nodes = 0.5 * np.cos((np.arange(64) + 0.5) * np.pi / 128)
    powers = np.stack([nodes, nodes**3, nodes**5], axis=1)
    wanted = 2.0**0.75 * np.sin(0.5 * np.pi * nodes)
    return [float(c) for c in np.linalg.lstsq(powers, wanted, rcond=None)[0]]


C0, C1, C2 = half_turn_coefficients()


def group_members(mesh, bit):
    n_rows, n_cols = mesh.shape["sx"], mesh.shape["sy"]
    step = 1 << bit
    groups = []
    for row in range(n_rows):
        for col in range(n_cols):
            if not row & step and not col & step:
                groups.append(
                    [(row + a) * n_cols + col + c for a in (0, step) for c in (0, step)]
                )
    return groups


def swapped(block, axis):
    count = lax.axis_size(axis)
    return lax.ppermute(block, axis, [(i, i ^ 1) for i in range(count)])


def fetch(pairs, sems):
    copies = [pltpu.make_async_copy(a, b, sems.at[i]) for i, (a, b) in enumerate(pairs)]
    for copy in copies:
        copy.start()
    return copies


def own_position(level):
    step = 1 << level
    row = lax.axis_index("sx") // step % 2
    col = lax.axis_index("sy") // step % 2
    return 2 * row + col


def spread_matrices(rows, cols, row_ref, col_ref):
    lane = lax.broadcasted_iota(jnp.int32, (CHEB, NODES), 1)
    node = lax.broadcasted_iota(jnp.int32, (CHEB, NODES), 0)
    outer = (lane // CHEB == node).astype(jnp.float32)
    inner = (lane % CHEB == node).astype(jnp.float32)
    spread = functools.partial(
        lax.dot_general,
        dimension_numbers=(((0,), (0,)), ((), ())),
        precision=lax.Precision.HIGHEST,
        preferred_element_type=jnp.float32,
    )
    for bit in range(2):
        row_ref[bit] = spread(rows[bit], outer)
        col_ref[bit] = spread(cols[bit], inner)


def normalize(matrices, normal, level):
    for bit in range(2):
        values = matrices[bit]
        top = jnp.max(jnp.abs(values), axis=(0, 1), keepdims=True)
        safe = jnp.where(top > 0.0, top, 1.0)
        normal[bit] = values / safe
        level[pl.ds(bit, 1), :] = jnp.broadcast_to(safe, (1, 128))


def spread_sources(source, a_ref, b_ref):
    lines = []
    for box in range(BOXES):
        freq = source(0, box)
        slow = source(1, box)
        near = 16.0 * freq * freq
        lines += [near, near * slow * slow]
    columns = jnp.concatenate(lines + lines, axis=0).T
    for box in range(BOXES):
        a_ref[box] = jnp.broadcast_to(columns[:, 2 * box : 2 * box + 1], (NODES, 128))
        b_ref[box] = jnp.broadcast_to(columns[:, 2 * box + 1 : 2 * box + 2], (NODES, 128))


def prepare(sources, rows, cols, tables):
    a_ref, b_ref, row_ref, col_ref = tables
    spread_matrices(rows, cols, row_ref, col_ref)
    spread_sources(lambda kind, box: sources[kind, box], a_ref, b_ref)


def line_of(targets):
    return lambda kind, row_bit, col_bit, box: targets[kind, row_bit, col_bit, box]


def weigh(position, box, target, tables, high, low):
    a_ref, b_ref, row_ref, col_ref = tables
    row_bit, col_bit = position // 2, position % 2
    tau = target(0, row_bit, col_bit, box)
    off = target(1, row_bit, col_bit, box)
    tau2, off2 = tau * tau, off * off
    inner = col_ref[col_bit]
    for step in range(CHEB):
        down = pl.ds(step * CHEB, CHEB)
        along = pl.ds(NODES + step * CHEB, CHEB)
        near = a_ref[box, down, :]
        far = b_ref[box, down, :]
        near = jnp.concatenate([near, near], axis=1)
        far = jnp.concatenate([far, far], axis=1)
        kron = row_ref[row_bit, pl.ds(step, 1), :] * inner
        z = near * tau2 + far * off2
        turns = z * lax.rsqrt(z)
        rest = turns - jnp.round(turns)
        y = rest * rest
        half = rest * (C0 + y * (C1 + y * C2))
        q = half * half
        cosine = ROOT2 - q
        v = 2.0 * ROOT2 - q
        sine = half * (v * lax.rsqrt(v))
        part = kron * sine
        real = kron - part * sine
        imag = part * cosine
        for where, value in ((down, real), (along, imag)):
            top = value.astype(jnp.bfloat16)
            high[where, :] = top
            rest_of = value - top.astype(jnp.float32)
            if low.dtype != jnp.bfloat16:
                rest_of = rest_of * LOW_SCALE
            low[where, :] = rest_of.astype(low.dtype)


def stacked(values):
    def turned(x):
        return jnp.concatenate([-x[RHS:], x[:RHS]], axis=0)

    top = values.astype(jnp.bfloat16)
    rest = (values - top.astype(jnp.float32)).astype(jnp.bfloat16)
    left = jnp.concatenate([top, rest], axis=0)
    right = jnp.concatenate([turned(top), turned(rest)], axis=0)
    return jnp.concatenate([left, right], axis=1)


def stack_boxes(real, imag, left):
    for box in range(BOXES):
        left[box] = stacked(jnp.concatenate([real[box], imag[box]], axis=0))


def product(left, high, low):
    main = jnp.dot(left, high, preferred_element_type=jnp.float32)
    scaled = low.dtype != jnp.bfloat16
    small = jnp.dot(
        left[: 2 * RHS], low, preferred_element_type=jnp.float32
    )
    if scaled:
        small = small * (1.0 / LOW_SCALE)
    return main[: 2 * RHS] + main[2 * RHS :] + small


def put(out, index, box, total):
    out[index, 0, box] = total[:RHS]
    out[index, 1, box] = total[RHS:]


def packed_source(packed):
    return lambda kind, box: packed[pl.ds(SOURCE_LINE + 2 * kind + box, 1), :]


def packed_target(packed):
    def line(kind, row_bit, col_bit, box):
        place = ((kind * 2 + row_bit) * 2 + col_bit) * BOXES + box
        return packed[pl.ds(TARGET_LINE + place, 1), :]

    return line


def packed_values(packed, box):
    real = packed[box * RHS : (box + 1) * RHS, :]
    imag = packed[(BOXES + box) * RHS : (BOXES + box + 1) * RHS, :]
    return jnp.concatenate([real, imag], axis=0)


def pack_kernel(
    coeffs_hbm, sources_hbm, targets_hbm, rows_hbm, cols_hbm, packed, rows, cols,
    coeffs, sources, targets, sems,
):
    copies = fetch(
        [
            (coeffs_hbm, coeffs),
            (sources_hbm.at[0], sources),
            (targets_hbm.at[0], targets),
            (rows_hbm.at[0], rows),
            (cols_hbm.at[0], cols),
        ],
        sems,
    )
    for copy in copies:
        copy.wait()
    for part in range(2):
        for box in range(BOXES):
            packed[pl.ds((part * BOXES + box) * RHS, RHS), :] = coeffs[part, box]
    lines = [sources[kind, box] for kind in range(2) for box in range(BOXES)]
    for kind in range(2):
        for place in range(4 * BOXES):
            lines.append(targets[kind, place // 4, place // 2 % 2, place % 2])
    lines += [lines[-1]] * (PACKED - SOURCE_LINE - len(lines))
    packed[pl.ds(SOURCE_LINE, PACKED - SOURCE_LINE), :] = jnp.concatenate(lines, axis=0)


def pair_of_boxes(packed, position, tables, high, low):
    target = packed_target(packed)
    for box in range(BOXES):
        weigh(position, box, target, tables, high.at[box], low.at[box])
    return [
        product(stacked(packed_values(packed, box)), high[box], low[box]) for box in range(BOXES)
    ]


def near_kernel(packed, rows, cols, partial, row_ref, col_ref, a_ref, b_ref, high, low):
    spread_matrices(rows, cols, row_ref, col_ref)
    spread_sources(packed_source(packed), a_ref, b_ref)
    tables = (a_ref, b_ref, row_ref, col_ref)
    both = pair_of_boxes(packed, own_position(0) ^ 2, tables, high, low)
    for box in range(BOXES):
        partial[0, box] = both[box][:RHS]
        partial[1, box] = both[box][RHS:]


def partner_kernel(packed, row_ref, col_ref, partial, sent, a_ref, b_ref, high, low):
    spread_sources(packed_source(packed), a_ref, b_ref)
    tables = (a_ref, b_ref, row_ref, col_ref)
    both = pair_of_boxes(packed, own_position(0) ^ 2, tables, high, low)
    for box in range(BOXES):
        sent[0, box] = partial[0, box] + both[box][:RHS]
        sent[1, box] = partial[1, box] + both[box][RHS:]


def make_weights(level, first, targets, tables, high, low):
    there = own_position(level)

    def make(step, carry):
        for box in range(BOXES):
            item = BOXES * step + box
            weigh(
                there ^ (step + first), box, line_of(targets), tables, high.at[item], low.at[item]
            )
        return carry

    lax.fori_loop(0, 4 - first, make, 0)


def second_kernel(
    packed, got, row0_ref, col0_ref, a_near, b_near, a_got, b_got,
    sources_hbm, targets_hbm, rows_hbm, cols_hbm,
    own, high, low,
    sources, targets, rows, cols, a_ref, b_ref, row_ref, col_ref, own_high, own_low, sems,
):
    nodes = fetch(
        [
            (sources_hbm.at[1], sources),
            (rows_hbm.at[1], rows),
            (cols_hbm.at[1], cols),
            (targets_hbm.at[1], targets),
        ],
        sems,
    )
    me = own_position(0)
    halves = [
        pair_of_boxes(lines, me, (a0, b0, row0_ref, col0_ref), own_high, own_low)
        for lines, a0, b0 in ((packed, a_near, b_near), (got, a_got, b_got))
    ]
    for box in range(BOXES):
        total = halves[0][box] + halves[1][box]
        own[0, box] = total[:RHS]
        own[1, box] = total[RHS:]
    for copy in nodes:
        copy.wait()
    tables = (a_ref, b_ref, row_ref, col_ref)
    prepare(sources, rows, cols, tables)
    make_weights(1, 1, targets, tables, high, low)


def between_kernel(
    values, sources_hbm, targets_hbm, rows_hbm, cols_hbm, own, high, low, row_size, col_size,
    sources, targets, rows, cols, *rest,
):
    *tables, own_high, own_low, left, row_normal, col_normal, sems = rest
    here = pl.ds(1, 2)
    nodes = fetch(
        [
            (sources_hbm.at[here], sources),
            (rows_hbm.at[here], rows),
            (cols_hbm.at[here], cols),
            (targets_hbm.at[here], targets),
        ],
        sems,
    )
    stack_boxes(values[0], values[1], left)
    for copy in nodes:
        copy.wait()
    prepare(sources.at[0], rows.at[0], cols.at[0], tables)
    me = own_position(1)

    for box in range(BOXES):
        weigh(me, box, line_of(targets.at[0]), tables, own_high.at[box], own_low.at[box])
    for box in range(BOXES):
        total = product(left[box], own_high[box], own_low[box])
        own[0, box] = total[:RHS]
        own[1, box] = total[RHS:]
    normalize(rows.at[1], row_normal, row_size)
    normalize(cols.at[1], col_normal, col_size)
    prepare(sources.at[1], row_normal, col_normal, tables)
    make_weights(2, 0, targets.at[1], tables, high, low)


def middle_kernel(piece, own, high, low, out_hbm, current, left, stage, sems):
    values = own[...] + piece[...]
    current[...] = values
    stack_boxes(values[0], values[1], left)
    me = own_position(1)
    sent = []
    for x in range(FOREIGN):
        for box in range(BOXES):
            item = 2 * x + box
            put(stage, x, box, product(left[box], high[item], low[item]))
        copy = pltpu.make_async_copy(stage.at[x], out_hbm.at[me ^ (x + 1)], sems.at[x])
        copy.start()
        sent.append(copy)
    for copy in sent:
        copy.wait()


def late_kernel(pieces, own, high, low, row_size, col_size, out, left):
    me = own_position(1)
    values = (own[...] + pieces[me ^ 1]) + (pieces[me ^ 2] + pieces[me ^ 3])
    stack_boxes(values[0], values[1], left)
    there = own_position(2)
    for x in range(4):
        place = there ^ x
        size = row_size[pl.ds(place // 2, 1), :] * col_size[pl.ds(place % 2, 1), :]
        size = jnp.concatenate([size, size], axis=1)
        for box in range(BOXES):
            item = 2 * x + box
            put(out, place, box, product(left[box], high[item], low[item]) * size)


def final_kernel(pieces, out):
    out[...] = (pieces[0] + pieces[1]) + (pieces[2] + pieces[3])


def node_buffers(count):
    lead = () if count is None else (count,)
    return (
        pltpu.VMEM(lead + (2, BOXES, 1, NODES), jnp.float32),
        pltpu.VMEM(lead + (2, 2, 2, BOXES, 1, NODES), jnp.float32),
        pltpu.VMEM(lead + (2, CHEB, CHEB), jnp.float32),
        pltpu.VMEM(lead + (2, CHEB, CHEB), jnp.float32),
    )


TABLES = (
    pltpu.VMEM((BOXES, NODES, 128), jnp.float32),
    pltpu.VMEM((BOXES, NODES, 128), jnp.float32),
    pltpu.VMEM((2, CHEB, NODES), jnp.float32),
    pltpu.VMEM((2, CHEB, NODES), jnp.float32),
)
FIELD = (2, BOXES, RHS, NODES)
LEFT = pltpu.VMEM((BOXES, 4 * RHS, 2 * NODES), jnp.bfloat16)
STAGE = pltpu.VMEM((FOREIGN,) + FIELD, jnp.float32)
ANY = pl.BlockSpec(memory_space=pltpu.HBM)
WHOLE = pl.BlockSpec(memory_space=pltpu.VMEM)
PARAMS = pltpu.CompilerParams(vmem_limit_bytes=12 * 1024 * 1024)


SENT = pltpu.HBM((4,) + FIELD, jnp.float32)
KEPT = pltpu.VMEM(FIELD, jnp.float32)
SPREAD = pltpu.VMEM((2, CHEB, NODES), jnp.float32)
SMALL = pltpu.VMEM((2, CHEB, CHEB), jnp.float32)
PAIR = pltpu.VMEM((BOXES, 2 * NODES, NODES), jnp.bfloat16)
COLUMNS = pltpu.VMEM((BOXES, NODES, 128), jnp.float32)
MADE = pltpu.VMEM((ITEMS, 2 * NODES, NODES), jnp.bfloat16)


def far(x):
    return pltpu.with_memory_space_constraint(x, pltpu.HBM)


def cost(flops):
    return pl.CostEstimate(flops=flops, bytes_accessed=100_000, transcendentals=0)


def solution(mesh):
    groups = [group_members(mesh, bit) for bit in range(LEVELS)]

    def exchange(sent, level):
        return lax.all_to_all(
            sent, ("sx", "sy"), 0, 0, axis_index_groups=groups[level], tiled=True
        )

    def local(coeffs, source_nodes, target_nodes, interp_rows, interp_cols):
        current = coeffs.reshape(FIELD)
        nodes = (
            far(source_nodes.reshape(LEVELS, 2, BOXES, 1, NODES)),
            far(target_nodes.reshape(LEVELS, 2, 2, 2, BOXES, 1, NODES)),
            far(interp_rows),
            far(interp_cols),
        )
        packed, rows, cols = pl.pallas_call(
            pack_kernel,
            in_specs=[ANY] * 5,
            out_specs=[WHOLE] * 3,
            out_shape=[pltpu.VMEM((PACKED, NODES), jnp.float32), SMALL, SMALL],
            scratch_shapes=(KEPT,) + node_buffers(None)[:2] + (pltpu.SemaphoreType.DMA((5,)),),
            compiler_params=PARAMS,
            name="pack",
        )(far(current), *nodes)
        got = swapped(packed, "sy")
        partial, row0, col0, a_near, b_near = pl.pallas_call(
            near_kernel,
            in_specs=[WHOLE] * 3,
            out_specs=[WHOLE] * 5,
            out_shape=[KEPT, SPREAD, SPREAD, COLUMNS, COLUMNS],
            scratch_shapes=(PAIR, PAIR),
            compiler_params=PARAMS,
            cost_estimate=cost(20_000_000),
            name="near",
        )(packed, rows, cols)
        sent, a_got, b_got = pl.pallas_call(
            partner_kernel,
            in_specs=[WHOLE] * 4,
            out_specs=[WHOLE] * 3,
            out_shape=[KEPT, COLUMNS, COLUMNS],
            scratch_shapes=(PAIR, PAIR),
            compiler_params=PARAMS,
            name="partner",
        )(got, row0, col0, partial)
        own, high, low = pl.pallas_call(
            second_kernel,
            in_specs=[WHOLE] * 8 + [ANY] * 4,
            out_specs=[WHOLE] * 3,
            out_shape=[KEPT, MADE, MADE],
            scratch_shapes=node_buffers(None)
            + TABLES
            + (PAIR, PAIR, pltpu.SemaphoreType.DMA((4,))),
            compiler_params=PARAMS,
            cost_estimate=cost(60_000_000),
            name="second",
        )(packed, got, row0, col0, a_near, b_near, a_got, b_got, *nodes)
        pieces = swapped(sent, "sx")
        sent, current = pl.pallas_call(
            middle_kernel,
            in_specs=[WHOLE] * 4,
            out_specs=[ANY, WHOLE],
            out_shape=[SENT, KEPT],
            scratch_shapes=(LEFT, STAGE, pltpu.SemaphoreType.DMA((FOREIGN,))),
            compiler_params=PARAMS,
            name="middle",
        )(pieces, own, high, low)
        made = pl.pallas_call(
            between_kernel,
            in_specs=[WHOLE] + [ANY] * 4,
            out_specs=[WHOLE] * 5,
            out_shape=[
                KEPT,
                pltpu.VMEM((4 * BOXES, 2 * NODES, NODES), jnp.bfloat16),
                pltpu.VMEM((4 * BOXES, 2 * NODES, NODES), jnp.float8_e4m3fn),
                pltpu.VMEM((2, 128), jnp.float32),
                pltpu.VMEM((2, 128), jnp.float32),
            ],
            scratch_shapes=node_buffers(2)
            + TABLES
            + (PAIR, PAIR, LEFT, SMALL, SMALL, pltpu.SemaphoreType.DMA((4,))),
            compiler_params=PARAMS,
            cost_estimate=cost(60_000_000),
            name="between",
        )(current, *nodes)
        pieces = exchange(sent, 1)
        sent = pl.pallas_call(
            late_kernel,
            in_specs=[WHOLE] * 6,
            out_specs=WHOLE,
            out_shape=pltpu.VMEM((4,) + FIELD, jnp.float32),
            scratch_shapes=(LEFT,),
            compiler_params=PARAMS,
            name="late",
        )(pieces, *made)
        field = pl.pallas_call(
            final_kernel,
            in_specs=[WHOLE],
            out_specs=WHOLE,
            out_shape=jax.ShapeDtypeStruct(FIELD, jnp.float32),
            compiler_params=PARAMS,
            name="final",
        )(exchange(sent, 2))
        return field.reshape(2, BOXES, 1, RHS, NODES)

    in_specs = (
        P(None, "sx", "sy", None, None),
        P(None, None, "sx", "sy", None),
        P(None, None, None, None, "sx", "sy", None),
        P(),
        P(),
    )
    out_specs = P(None, "sx", "sy", None, None)
    return jax.shard_map(local, mesh=mesh, in_specs=in_specs, out_specs=out_specs, check_vma=False)
```

```python
import functools
import math

import jax
import jax.numpy as jnp
import numpy as np
from jax import lax
from jax.experimental import pallas as pl
from jax.experimental.pallas import tpu as pltpu
from jax.sharding import PartitionSpec as P

LEVELS = 3
CHEB = 16
NODES = CHEB * CHEB
RHS = 16
BOXES = 2
FOREIGN = 3
ITEMS = FOREIGN * BOXES
ROOT2 = math.sqrt(2.0)
SOURCE_LINE = 2 * BOXES * RHS
TARGET_LINE = SOURCE_LINE + 2 * BOXES
PACKED = 88
LOW_SCALE = 2.0**17


def half_turn_coefficients():
    nodes = 0.5 * np.cos((np.arange(64) + 0.5) * np.pi / 128)
    powers = np.stack([nodes, nodes**3, nodes**5], axis=1)
    wanted = 2.0**0.75 * np.sin(0.5 * np.pi * nodes)
    return [float(c) for c in np.linalg.lstsq(powers, wanted, rcond=None)[0]]


C0, C1, C2 = half_turn_coefficients()


def group_members(mesh, bit):
    n_rows, n_cols = mesh.shape["sx"], mesh.shape["sy"]
    step = 1 << bit
    groups = []
    for row in range(n_rows):
        for col in range(n_cols):
            if not row & step and not col & step:
                groups.append(
                    [(row + a) * n_cols + col + c for a in (0, step) for c in (0, step)]
                )
    return groups


def swapped(block, axis):
    count = lax.axis_size(axis)
    return lax.ppermute(block, axis, [(i, i ^ 1) for i in range(count)])


def fetch(pairs, sems):
    copies = [pltpu.make_async_copy(a, b, sems.at[i]) for i, (a, b) in enumerate(pairs)]
    for copy in copies:
        copy.start()
    return copies


def own_position(level):
    step = 1 << level
    row = lax.axis_index("sx") // step % 2
    col = lax.axis_index("sy") // step % 2
    return 2 * row + col


def spread_matrices(rows, cols, row_ref, col_ref):
    lane = lax.broadcasted_iota(jnp.int32, (CHEB, NODES), 1)
    node = lax.broadcasted_iota(jnp.int32, (CHEB, NODES), 0)
    outer = (lane // CHEB == node).astype(jnp.float32)
    inner = (lane % CHEB == node).astype(jnp.float32)
    spread = functools.partial(
        lax.dot_general,
        dimension_numbers=(((0,), (0,)), ((), ())),
        precision=lax.Precision.HIGHEST,
        preferred_element_type=jnp.float32,
    )
    for bit in range(2):
        row_ref[bit] = spread(rows[bit], outer)
        col_ref[bit] = spread(cols[bit], inner)


def normalize(matrices, normal, level):
    for bit in range(2):
        values = matrices[bit]
        top = jnp.max(jnp.abs(values), axis=(0, 1), keepdims=True)
        safe = jnp.where(top > 0.0, top, 1.0)
        normal[bit] = values / safe
        level[pl.ds(bit, 1), :] = jnp.broadcast_to(safe, (1, 128))


def spread_sources(source, a_ref, b_ref):
    lines = []
    for box in range(BOXES):
        freq = source(0, box)
        slow = source(1, box)
        near = 16.0 * freq * freq
        lines += [near, near * slow * slow]
    columns = jnp.concatenate(lines + lines, axis=0).T
    for box in range(BOXES):
        a_ref[box] = jnp.broadcast_to(columns[:, 2 * box : 2 * box + 1], (NODES, 128))
        b_ref[box] = jnp.broadcast_to(columns[:, 2 * box + 1 : 2 * box + 2], (NODES, 128))


def prepare(sources, rows, cols, tables):
    a_ref, b_ref, row_ref, col_ref = tables
    spread_matrices(rows, cols, row_ref, col_ref)
    spread_sources(lambda kind, box: sources[kind, box], a_ref, b_ref)


def line_of(targets):
    return lambda kind, row_bit, col_bit, box: targets[kind, row_bit, col_bit, box]


def weigh(position, box, target, tables, high, low):
    a_ref, b_ref, row_ref, col_ref = tables
    row_bit, col_bit = position // 2, position % 2
    tau = target(0, row_bit, col_bit, box)
    off = target(1, row_bit, col_bit, box)
    tau2, off2 = tau * tau, off * off
    inner = col_ref[col_bit]
    for step in range(CHEB):
        down = pl.ds(step * CHEB, CHEB)
        along = pl.ds(NODES + step * CHEB, CHEB)
        near = a_ref[box, down, :]
        far = b_ref[box, down, :]
        near = jnp.concatenate([near, near], axis=1)
        far = jnp.concatenate([far, far], axis=1)
        kron = row_ref[row_bit, pl.ds(step, 1), :] * inner
        z = near * tau2 + far * off2
        turns = z * lax.rsqrt(z)
        rest = turns - jnp.round(turns)
        y = rest * rest
        half = rest * (C0 + y * (C1 + y * C2))
        q = half * half
        cosine = ROOT2 - q
        v = 2.0 * ROOT2 - q
        sine = half * (v * lax.rsqrt(v))
        part = kron * sine
        real = kron - part * sine
        imag = part * cosine
        for where, value in ((down, real), (along, imag)):
            top = value.astype(jnp.bfloat16)
            high[where, :] = top
            rest_of = value - top.astype(jnp.float32)
            if low.dtype != jnp.bfloat16:
                rest_of = rest_of * LOW_SCALE
            low[where, :] = rest_of.astype(low.dtype)


def stacked(values):
    def turned(x):
        return jnp.concatenate([-x[RHS:], x[:RHS]], axis=0)

    top = values.astype(jnp.bfloat16)
    rest = (values - top.astype(jnp.float32)).astype(jnp.bfloat16)
    left = jnp.concatenate([top, rest], axis=0)
    right = jnp.concatenate([turned(top), turned(rest)], axis=0)
    return jnp.concatenate([left, right], axis=1)


def stack_boxes(real, imag, left):
    for box in range(BOXES):
        left[box] = stacked(jnp.concatenate([real[box], imag[box]], axis=0))


def product(left, high, low):
    main = jnp.dot(left, high, preferred_element_type=jnp.float32)
    scaled = low.dtype != jnp.bfloat16
    small = jnp.dot(
        left[: 2 * RHS], low, preferred_element_type=jnp.float32
    )
    if scaled:
        small = small * (1.0 / LOW_SCALE)
    return main[: 2 * RHS] + main[2 * RHS :] + small


def put(out, index, box, total):
    out[index, 0, box] = total[:RHS]
    out[index, 1, box] = total[RHS:]


def packed_source(packed):
    return lambda kind, box: packed[pl.ds(SOURCE_LINE + 2 * kind + box, 1), :]


def packed_target(packed):
    def line(kind, row_bit, col_bit, box):
        place = ((kind * 2 + row_bit) * 2 + col_bit) * BOXES + box
        return packed[pl.ds(TARGET_LINE + place, 1), :]

    return line


def packed_values(packed, box):
    real = packed[box * RHS : (box + 1) * RHS, :]
    imag = packed[(BOXES + box) * RHS : (BOXES + box + 1) * RHS, :]
    return jnp.concatenate([real, imag], axis=0)


def pack_kernel(
    coeffs_hbm, sources_hbm, targets_hbm, rows_hbm, cols_hbm, packed, rows, cols,
    coeffs, sources, targets, sems,
):
    copies = fetch(
        [
            (coeffs_hbm, coeffs),
            (sources_hbm.at[0], sources),
            (targets_hbm.at[0], targets),
            (rows_hbm.at[0], rows),
            (cols_hbm.at[0], cols),
        ],
        sems,
    )
    for copy in copies:
        copy.wait()
    for part in range(2):
        for box in range(BOXES):
            packed[pl.ds((part * BOXES + box) * RHS, RHS), :] = coeffs[part, box]
    lines = [sources[kind, box] for kind in range(2) for box in range(BOXES)]
    for kind in range(2):
        for place in range(4 * BOXES):
            lines.append(targets[kind, place // 4, place // 2 % 2, place % 2])
    lines += [lines[-1]] * (PACKED - SOURCE_LINE - len(lines))
    packed[pl.ds(SOURCE_LINE, PACKED - SOURCE_LINE), :] = jnp.concatenate(lines, axis=0)


def pair_of_boxes(packed, position, tables, high, low):
    target = packed_target(packed)
    for box in range(BOXES):
        weigh(position, box, target, tables, high.at[box], low.at[box])
    return [
        product(stacked(packed_values(packed, box)), high[box], low[box]) for box in range(BOXES)
    ]


def near_kernel(packed, rows, cols, partial, row_ref, col_ref, a_ref, b_ref, high, low):
    spread_matrices(rows, cols, row_ref, col_ref)
    spread_sources(packed_source(packed), a_ref, b_ref)
    tables = (a_ref, b_ref, row_ref, col_ref)
    both = pair_of_boxes(packed, own_position(0) ^ 2, tables, high, low)
    for box in range(BOXES):
        partial[0, box] = both[box][:RHS]
        partial[1, box] = both[box][RHS:]


def partner_kernel(packed, row_ref, col_ref, partial, sent, a_ref, b_ref, high, low):
    spread_sources(packed_source(packed), a_ref, b_ref)
    tables = (a_ref, b_ref, row_ref, col_ref)
    both = pair_of_boxes(packed, own_position(0) ^ 2, tables, high, low)
    for box in range(BOXES):
        sent[0, box] = partial[0, box] + both[box][:RHS]
        sent[1, box] = partial[1, box] + both[box][RHS:]


def make_weights(level, first, targets, tables, high, low):
    there = own_position(level)

    def make(step, carry):
        for box in range(BOXES):
            item = BOXES * step + box
            weigh(
                there ^ (step + first), box, line_of(targets), tables, high.at[item], low.at[item]
            )
        return carry

    lax.fori_loop(0, 4 - first, make, 0)


def second_kernel(
    packed, got, row0_ref, col0_ref, a_near, b_near, a_got, b_got,
    sources_hbm, targets_hbm, rows_hbm, cols_hbm,
    own, high, low,
    sources, targets, rows, cols, a_ref, b_ref, row_ref, col_ref, own_high, own_low, sems,
):
    nodes = fetch(
        [
            (sources_hbm.at[1], sources),
            (rows_hbm.at[1], rows),
            (cols_hbm.at[1], cols),
            (targets_hbm.at[1], targets),
        ],
        sems,
    )
    me = own_position(0)
    places = ((packed, a_near, b_near), (got, a_got, b_got))

    def mine(box, carry):
        for index, (lines, a0, b0) in enumerate(places):
            tables = (a0, b0, row0_ref, col0_ref)
            weigh(me, box, packed_target(lines), tables, own_high.at[index], own_low.at[index])
        total = 0.0
        for index, (lines, a0, b0) in enumerate(places):
            start = pl.multiple_of(box * RHS, RHS)
            real = lines[pl.ds(start, RHS), :]
            imag = lines[pl.ds(start + BOXES * RHS, RHS), :]
            left = stacked(jnp.concatenate([real, imag], axis=0))
            total = total + product(left, own_high[index], own_low[index])
        own[0, box] = total[:RHS]
        own[1, box] = total[RHS:]
        return carry

    lax.fori_loop(0, BOXES, mine, 0)
    for copy in nodes:
        copy.wait()
    tables = (a_ref, b_ref, row_ref, col_ref)
    prepare(sources, rows, cols, tables)
    make_weights(1, 1, targets, tables, high, low)


def between_kernel(
    values, sources_hbm, targets_hbm, rows_hbm, cols_hbm, own, high, low, row_size, col_size,
    sources, targets, rows, cols, *rest,
):
    *tables, own_high, own_low, left, row_normal, col_normal, sems = rest
    here = pl.ds(1, 2)
    nodes = fetch(
        [
            (sources_hbm.at[here], sources),
            (rows_hbm.at[here], rows),
            (cols_hbm.at[here], cols),
            (targets_hbm.at[here], targets),
        ],
        sems,
    )
    stack_boxes(values[0], values[1], left)
    for copy in nodes:
        copy.wait()
    prepare(sources.at[0], rows.at[0], cols.at[0], tables)
    me = own_position(1)

    for box in range(BOXES):
        weigh(me, box, line_of(targets.at[0]), tables, own_high.at[box], own_low.at[box])
    for box in range(BOXES):
        total = product(left[box], own_high[box], own_low[box])
        own[0, box] = total[:RHS]
        own[1, box] = total[RHS:]
    normalize(rows.at[1], row_normal, row_size)
    normalize(cols.at[1], col_normal, col_size)
    prepare(sources.at[1], row_normal, col_normal, tables)
    make_weights(2, 0, targets.at[1], tables, high, low)


def middle_kernel(piece, own, high, low, out_hbm, current, left, stage, sems):
    values = own[...] + piece[...]
    current[...] = values
    stack_boxes(values[0], values[1], left)
    me = own_position(1)
    sent = []
    for x in range(FOREIGN):
        for box in range(BOXES):
            item = 2 * x + box
            put(stage, x, box, product(left[box], high[item], low[item]))
        copy = pltpu.make_async_copy(stage.at[x], out_hbm.at[me ^ (x + 1)], sems.at[x])
        copy.start()
        sent.append(copy)
    for copy in sent:
        copy.wait()


def late_kernel(pieces, own, high, low, row_size, col_size, out, left):
    me = own_position(1)
    values = (own[...] + pieces[me ^ 1]) + (pieces[me ^ 2] + pieces[me ^ 3])
    stack_boxes(values[0], values[1], left)
    there = own_position(2)
    for x in range(4):
        place = there ^ x
        size = row_size[pl.ds(place // 2, 1), :] * col_size[pl.ds(place % 2, 1), :]
        size = jnp.concatenate([size, size], axis=1)
        for box in range(BOXES):
            item = 2 * x + box
            put(out, place, box, product(left[box], high[item], low[item]) * size)


def final_kernel(pieces, out):
    out[...] = (pieces[0] + pieces[1]) + (pieces[2] + pieces[3])


def node_buffers(count):
    lead = () if count is None else (count,)
    return (
        pltpu.VMEM(lead + (2, BOXES, 1, NODES), jnp.float32),
        pltpu.VMEM(lead + (2, 2, 2, BOXES, 1, NODES), jnp.float32),
        pltpu.VMEM(lead + (2, CHEB, CHEB), jnp.float32),
        pltpu.VMEM(lead + (2, CHEB, CHEB), jnp.float32),
    )


TABLES = (
    pltpu.VMEM((BOXES, NODES, 128), jnp.float32),
    pltpu.VMEM((BOXES, NODES, 128), jnp.float32),
    pltpu.VMEM((2, CHEB, NODES), jnp.float32),
    pltpu.VMEM((2, CHEB, NODES), jnp.float32),
)
FIELD = (2, BOXES, RHS, NODES)
LEFT = pltpu.VMEM((BOXES, 4 * RHS, 2 * NODES), jnp.bfloat16)
STAGE = pltpu.VMEM((FOREIGN,) + FIELD, jnp.float32)
ANY = pl.BlockSpec(memory_space=pltpu.HBM)
WHOLE = pl.BlockSpec(memory_space=pltpu.VMEM)
PARAMS = pltpu.CompilerParams(vmem_limit_bytes=12 * 1024 * 1024)


SENT = pltpu.HBM((4,) + FIELD, jnp.float32)
KEPT = pltpu.VMEM(FIELD, jnp.float32)
SPREAD = pltpu.VMEM((2, CHEB, NODES), jnp.float32)
SMALL = pltpu.VMEM((2, CHEB, CHEB), jnp.float32)
PAIR = pltpu.VMEM((BOXES, 2 * NODES, NODES), jnp.bfloat16)
COLUMNS = pltpu.VMEM((BOXES, NODES, 128), jnp.float32)
MADE = pltpu.VMEM((ITEMS, 2 * NODES, NODES), jnp.bfloat16)


def far(x):
    return pltpu.with_memory_space_constraint(x, pltpu.HBM)


def cost(flops):
    return pl.CostEstimate(flops=flops, bytes_accessed=100_000, transcendentals=0)


def solution(mesh):
    groups = [group_members(mesh, bit) for bit in range(LEVELS)]

    def exchange(sent, level):
        return lax.all_to_all(
            sent, ("sx", "sy"), 0, 0, axis_index_groups=groups[level], tiled=True
        )

    def local(coeffs, source_nodes, target_nodes, interp_rows, interp_cols):
        current = coeffs.reshape(FIELD)
        nodes = (
            far(source_nodes.reshape(LEVELS, 2, BOXES, 1, NODES)),
            far(target_nodes.reshape(LEVELS, 2, 2, 2, BOXES, 1, NODES)),
            far(interp_rows),
            far(interp_cols),
        )
        packed, rows, cols = pl.pallas_call(
            pack_kernel,
            in_specs=[ANY] * 5,
            out_specs=[WHOLE] * 3,
            out_shape=[pltpu.VMEM((PACKED, NODES), jnp.float32), SMALL, SMALL],
            scratch_shapes=(KEPT,) + node_buffers(None)[:2] + (pltpu.SemaphoreType.DMA((5,)),),
            compiler_params=PARAMS,
            name="pack",
        )(far(current), *nodes)
        got = swapped(packed, "sy")
        partial, row0, col0, a_near, b_near = pl.pallas_call(
            near_kernel,
            in_specs=[WHOLE] * 3,
            out_specs=[WHOLE] * 5,
            out_shape=[KEPT, SPREAD, SPREAD, COLUMNS, COLUMNS],
            scratch_shapes=(PAIR, PAIR),
            compiler_params=PARAMS,
            cost_estimate=cost(20_000_000),
            name="near",
        )(packed, rows, cols)
        sent, a_got, b_got = pl.pallas_call(
            partner_kernel,
            in_specs=[WHOLE] * 4,
            out_specs=[WHOLE] * 3,
            out_shape=[KEPT, COLUMNS, COLUMNS],
            scratch_shapes=(PAIR, PAIR),
            compiler_params=PARAMS,
            name="partner",
        )(got, row0, col0, partial)
        own, high, low = pl.pallas_call(
            second_kernel,
            in_specs=[WHOLE] * 8 + [ANY] * 4,
            out_specs=[WHOLE] * 3,
            out_shape=[KEPT, MADE, MADE],
            scratch_shapes=node_buffers(None)
            + TABLES
            + (PAIR, PAIR, pltpu.SemaphoreType.DMA((4,))),
            compiler_params=PARAMS,
            cost_estimate=cost(60_000_000),
            name="second",
        )(packed, got, row0, col0, a_near, b_near, a_got, b_got, *nodes)
        pieces = swapped(sent, "sx")
        sent, current = pl.pallas_call(
            middle_kernel,
            in_specs=[WHOLE] * 4,
            out_specs=[ANY, WHOLE],
            out_shape=[SENT, KEPT],
            scratch_shapes=(LEFT, STAGE, pltpu.SemaphoreType.DMA((FOREIGN,))),
            compiler_params=PARAMS,
            name="middle",
        )(pieces, own, high, low)
        made = pl.pallas_call(
            between_kernel,
            in_specs=[WHOLE] + [ANY] * 4,
            out_specs=[WHOLE] * 5,
            out_shape=[
                KEPT,
                pltpu.VMEM((4 * BOXES, 2 * NODES, NODES), jnp.bfloat16),
                pltpu.VMEM((4 * BOXES, 2 * NODES, NODES), jnp.float8_e4m3fn),
                pltpu.VMEM((2, 128), jnp.float32),
                pltpu.VMEM((2, 128), jnp.float32),
            ],
            scratch_shapes=node_buffers(2)
            + TABLES
            + (PAIR, PAIR, LEFT, SMALL, SMALL, pltpu.SemaphoreType.DMA((4,))),
            compiler_params=PARAMS,
            cost_estimate=cost(60_000_000),
            name="between",
        )(current, *nodes)
        pieces = exchange(sent, 1)
        sent = pl.pallas_call(
            late_kernel,
            in_specs=[WHOLE] * 6,
            out_specs=WHOLE,
            out_shape=pltpu.VMEM((4,) + FIELD, jnp.float32),
            scratch_shapes=(LEFT,),
            compiler_params=PARAMS,
            name="late",
        )(pieces, *made)
        field = pl.pallas_call(
            final_kernel,
            in_specs=[WHOLE],
            out_specs=WHOLE,
            out_shape=jax.ShapeDtypeStruct(FIELD, jnp.float32),
            compiler_params=PARAMS,
            name="final",
        )(exchange(sent, 2))
        return field.reshape(2, BOXES, 1, RHS, NODES)

    in_specs = (
        P(None, "sx", "sy", None, None),
        P(None, None, "sx", "sy", None),
        P(None, None, None, None, "sx", "sy", None),
        P(),
        P(),
    )
    out_specs = P(None, "sx", "sy", None, None)
    return jax.shard_map(local, mesh=mesh, in_specs=in_specs, out_specs=out_specs, check_vma=False)
```

```python
import functools
import math

import jax
import jax.numpy as jnp
import numpy as np
from jax import lax
from jax.experimental import pallas as pl
from jax.experimental.pallas import tpu as pltpu
from jax.sharding import PartitionSpec as P

LEVELS = 3
CHEB = 16
NODES = CHEB * CHEB
RHS = 16
BOXES = 2
FOREIGN = 3
ITEMS = FOREIGN * BOXES
ROOT2 = math.sqrt(2.0)
SOURCE_LINE = 2 * BOXES * RHS
TARGET_LINE = SOURCE_LINE + 2 * BOXES
PACKED = 88
LOW_SCALE = 2.0**17


def half_turn_coefficients():
    nodes = 0.5 * np.cos((np.arange(64) + 0.5) * np.pi / 128)
    powers = np.stack([nodes, nodes**3, nodes**5], axis=1)
    wanted = 2.0**0.75 * np.sin(0.5 * np.pi * nodes)
    return [float(c) for c in np.linalg.lstsq(powers, wanted, rcond=None)[0]]


C0, C1, C2 = half_turn_coefficients()


def group_members(mesh, bit):
    n_rows, n_cols = mesh.shape["sx"], mesh.shape["sy"]
    step = 1 << bit
    groups = []
    for row in range(n_rows):
        for col in range(n_cols):
            if not row & step and not col & step:
                groups.append(
                    [(row + a) * n_cols + col + c for a in (0, step) for c in (0, step)]
                )
    return groups


def swapped(block, axis):
    count = lax.axis_size(axis)
    return lax.ppermute(block, axis, [(i, i ^ 1) for i in range(count)])


def fetch(pairs, sems):
    copies = [pltpu.make_async_copy(a, b, sems.at[i]) for i, (a, b) in enumerate(pairs)]
    for copy in copies:
        copy.start()
    return copies


def own_position(level):
    step = 1 << level
    row = lax.axis_index("sx") // step % 2
    col = lax.axis_index("sy") // step % 2
    return 2 * row + col


def spread_matrices(rows, cols, row_ref, col_ref):
    lane = lax.broadcasted_iota(jnp.int32, (CHEB, NODES), 1)
    node = lax.broadcasted_iota(jnp.int32, (CHEB, NODES), 0)
    outer = (lane // CHEB == node).astype(jnp.float32)
    inner = (lane % CHEB == node).astype(jnp.float32)
    spread = functools.partial(
        lax.dot_general,
        dimension_numbers=(((0,), (0,)), ((), ())),
        precision=lax.Precision.HIGHEST,
        preferred_element_type=jnp.float32,
    )
    for bit in range(2):
        row_ref[bit] = spread(rows[bit], outer)
        col_ref[bit] = spread(cols[bit], inner)


def normalize(matrices, normal, level):
    for bit in range(2):
        values = matrices[bit]
        top = jnp.max(jnp.abs(values), axis=(0, 1), keepdims=True)
        safe = jnp.where(top > 0.0, top, 1.0)
        normal[bit] = values / safe
        level[pl.ds(bit, 1), :] = jnp.broadcast_to(safe, (1, 128))


def spread_sources(source, a_ref, b_ref):
    lines = []
    for box in range(BOXES):
        freq = source(0, box)
        slow = source(1, box)
        near = 16.0 * freq * freq
        lines += [near, near * slow * slow]
    columns = jnp.concatenate(lines + lines, axis=0).T
    for box in range(BOXES):
        a_ref[box] = jnp.broadcast_to(columns[:, 2 * box : 2 * box + 1], (NODES, 128))
        b_ref[box] = jnp.broadcast_to(columns[:, 2 * box + 1 : 2 * box + 2], (NODES, 128))


def prepare(sources, rows, cols, tables):
    a_ref, b_ref, row_ref, col_ref = tables
    spread_matrices(rows, cols, row_ref, col_ref)
    spread_sources(lambda kind, box: sources[kind, box], a_ref, b_ref)


def line_of(targets):
    return lambda kind, row_bit, col_bit, box: targets[kind, row_bit, col_bit, box]


def weigh(position, box, target, tables, high, low):
    a_ref, b_ref, row_ref, col_ref = tables
    row_bit, col_bit = position // 2, position % 2
    tau = target(0, row_bit, col_bit, box)
    off = target(1, row_bit, col_bit, box)
    tau2, off2 = tau * tau, off * off
    inner = col_ref[col_bit]
    for step in range(CHEB):
        down = pl.ds(step * CHEB, CHEB)
        along = pl.ds(NODES + step * CHEB, CHEB)
        near = a_ref[box, down, :]
        far = b_ref[box, down, :]
        near = jnp.concatenate([near, near], axis=1)
        far = jnp.concatenate([far, far], axis=1)
        kron = row_ref[row_bit, pl.ds(step, 1), :] * inner
        z = near * tau2 + far * off2
        turns = z * lax.rsqrt(z)
        rest = turns - jnp.round(turns)
        y = rest * rest
        half = rest * (C0 + y * (C1 + y * C2))
        q = half * half
        cosine = ROOT2 - q
        v = 2.0 * ROOT2 - q
        sine = half * (v * lax.rsqrt(v))
        part = kron * sine
        real = kron - part * sine
        imag = part * cosine
        for where, value in ((down, real), (along, imag)):
            top = value.astype(jnp.bfloat16)
            high[where, :] = top
            rest_of = value - top.astype(jnp.float32)
            if low.dtype != jnp.bfloat16:
                rest_of = rest_of * LOW_SCALE
            low[where, :] = rest_of.astype(low.dtype)


def stacked(values):
    def turned(x):
        return jnp.concatenate([-x[RHS:], x[:RHS]], axis=0)

    top = values.astype(jnp.bfloat16)
    rest = (values - top.astype(jnp.float32)).astype(jnp.bfloat16)
    left = jnp.concatenate([top, rest], axis=0)
    right = jnp.concatenate([turned(top), turned(rest)], axis=0)
    return jnp.concatenate([left, right], axis=1)


def stack_boxes(real, imag, left):
    for box in range(BOXES):
        left[box] = stacked(jnp.concatenate([real[box], imag[box]], axis=0))


def product(left, high, low):
    main = jnp.dot(left, high, preferred_element_type=jnp.float32)
    scaled = low.dtype != jnp.bfloat16
    small = jnp.dot(
        left[: 2 * RHS], low, preferred_element_type=jnp.float32
    )
    if scaled:
        small = small * (1.0 / LOW_SCALE)
    return main[: 2 * RHS] + main[2 * RHS :] + small


def put(out, index, box, total):
    out[index, 0, box] = total[:RHS]
    out[index, 1, box] = total[RHS:]


def packed_source(packed):
    return lambda kind, box: packed[pl.ds(SOURCE_LINE + 2 * kind + box, 1), :]


def packed_target(packed):
    def line(kind, row_bit, col_bit, box):
        place = ((kind * 2 + row_bit) * 2 + col_bit) * BOXES + box
        return packed[pl.ds(TARGET_LINE + place, 1), :]

    return line


def packed_values(packed, box):
    real = packed[box * RHS : (box + 1) * RHS, :]
    imag = packed[(BOXES + box) * RHS : (BOXES + box + 1) * RHS, :]
    return jnp.concatenate([real, imag], axis=0)


def pack_kernel(
    coeffs_hbm, sources_hbm, targets_hbm, rows_hbm, cols_hbm, packed, rows, cols,
    coeffs, sources, targets, sems,
):
    copies = fetch(
        [
            (coeffs_hbm, coeffs),
            (sources_hbm.at[0], sources),
            (targets_hbm.at[0], targets),
            (rows_hbm.at[0], rows),
            (cols_hbm.at[0], cols),
        ],
        sems,
    )
    for copy in copies:
        copy.wait()
    for part in range(2):
        for box in range(BOXES):
            packed[pl.ds((part * BOXES + box) * RHS, RHS), :] = coeffs[part, box]
    lines = [sources[kind, box] for kind in range(2) for box in range(BOXES)]
    for kind in range(2):
        for place in range(4 * BOXES):
            lines.append(targets[kind, place // 4, place // 2 % 2, place % 2])
    lines += [lines[-1]] * (PACKED - SOURCE_LINE - len(lines))
    packed[pl.ds(SOURCE_LINE, PACKED - SOURCE_LINE), :] = jnp.concatenate(lines, axis=0)


def pair_of_boxes(packed, position, tables, high, low):
    target = packed_target(packed)
    for box in range(BOXES):
        weigh(position, box, target, tables, high.at[box], low.at[box])
    return [
        product(stacked(packed_values(packed, box)), high[box], low[box]) for box in range(BOXES)
    ]


def near_kernel(
    packed, rows, cols, sources_hbm, targets_hbm, rows_hbm, cols_hbm,
    partial, row_ref, col_ref, a_ref, b_ref, a1_ref, b1_ref, row1_ref, col1_ref, targets1,
    high, low, sources1, rows1, cols1, sems,
):
    nodes = fetch(
        [
            (sources_hbm.at[1], sources1),
            (rows_hbm.at[1], rows1),
            (cols_hbm.at[1], cols1),
            (targets_hbm.at[1], targets1),
        ],
        sems,
    )
    spread_matrices(rows, cols, row_ref, col_ref)
    spread_sources(packed_source(packed), a_ref, b_ref)
    tables = (a_ref, b_ref, row_ref, col_ref)
    both = pair_of_boxes(packed, own_position(0) ^ 2, tables, high, low)
    for box in range(BOXES):
        partial[0, box] = both[box][:RHS]
        partial[1, box] = both[box][RHS:]
    for copy in nodes:
        copy.wait()
    prepare(sources1, rows1, cols1, (a1_ref, b1_ref, row1_ref, col1_ref))


def partner_kernel(packed, row_ref, col_ref, partial, sent, a_ref, b_ref, high, low):
    spread_sources(packed_source(packed), a_ref, b_ref)
    tables = (a_ref, b_ref, row_ref, col_ref)
    both = pair_of_boxes(packed, own_position(0) ^ 2, tables, high, low)
    for box in range(BOXES):
        sent[0, box] = partial[0, box] + both[box][:RHS]
        sent[1, box] = partial[1, box] + both[box][RHS:]


def make_weights(level, first, targets, tables, high, low):
    there = own_position(level)

    def make(step, carry):
        for box in range(BOXES):
            item = BOXES * step + box
            weigh(
                there ^ (step + first), box, line_of(targets), tables, high.at[item], low.at[item]
            )
        return carry

    lax.fori_loop(0, 4 - first, make, 0)


def second_kernel(
    packed, got, row0_ref, col0_ref, a_near, b_near, a_got, b_got,
    a_ref, b_ref, row_ref, col_ref, targets,
    own, high, low, own_high, own_low,
):
    me = own_position(0)
    places = ((packed, a_near, b_near), (got, a_got, b_got))

    def mine(box, carry):
        for index, (lines, a0, b0) in enumerate(places):
            tables = (a0, b0, row0_ref, col0_ref)
            weigh(me, box, packed_target(lines), tables, own_high.at[index], own_low.at[index])
        total = 0.0
        for index, (lines, a0, b0) in enumerate(places):
            start = pl.multiple_of(box * RHS, RHS)
            real = lines[pl.ds(start, RHS), :]
            imag = lines[pl.ds(start + BOXES * RHS, RHS), :]
            left = stacked(jnp.concatenate([real, imag], axis=0))
            total = total + product(left, own_high[index], own_low[index])
        own[0, box] = total[:RHS]
        own[1, box] = total[RHS:]
        return carry

    lax.fori_loop(0, BOXES, mine, 0)
    make_weights(1, 1, targets, (a_ref, b_ref, row_ref, col_ref), high, low)


def between_kernel(
    values, sources_hbm, targets_hbm, rows_hbm, cols_hbm, own, high, low, row_size, col_size,
    sources, targets, rows, cols, *rest,
):
    *tables, own_high, own_low, left, row_normal, col_normal, sems = rest
    here = pl.ds(1, 2)
    nodes = fetch(
        [
            (sources_hbm.at[here], sources),
            (rows_hbm.at[here], rows),
            (cols_hbm.at[here], cols),
            (targets_hbm.at[here], targets),
        ],
        sems,
    )
    stack_boxes(values[0], values[1], left)
    for copy in nodes:
        copy.wait()
    prepare(sources.at[0], rows.at[0], cols.at[0], tables)
    me = own_position(1)

    for box in range(BOXES):
        weigh(me, box, line_of(targets.at[0]), tables, own_high.at[box], own_low.at[box])
    for box in range(BOXES):
        total = product(left[box], own_high[box], own_low[box])
        own[0, box] = total[:RHS]
        own[1, box] = total[RHS:]
    normalize(rows.at[1], row_normal, row_size)
    normalize(cols.at[1], col_normal, col_size)
    prepare(sources.at[1], row_normal, col_normal, tables)
    make_weights(2, 0, targets.at[1], tables, high, low)


def middle_kernel(piece, own, high, low, out_hbm, current, left, stage, sems):
    values = own[...] + piece[...]
    current[...] = values
    stack_boxes(values[0], values[1], left)
    me = own_position(1)
    sent = []
    for x in range(FOREIGN):
        for box in range(BOXES):
            item = 2 * x + box
            put(stage, x, box, product(left[box], high[item], low[item]))
        copy = pltpu.make_async_copy(stage.at[x], out_hbm.at[me ^ (x + 1)], sems.at[x])
        copy.start()
        sent.append(copy)
    for copy in sent:
        copy.wait()


def late_kernel(pieces, own, high, low, row_size, col_size, out, left):
    me = own_position(1)
    values = (own[...] + pieces[me ^ 1]) + (pieces[me ^ 2] + pieces[me ^ 3])
    stack_boxes(values[0], values[1], left)
    there = own_position(2)
    for x in range(4):
        place = there ^ x
        size = row_size[pl.ds(place // 2, 1), :] * col_size[pl.ds(place % 2, 1), :]
        size = jnp.concatenate([size, size], axis=1)
        for box in range(BOXES):
            item = 2 * x + box
            put(out, place, box, product(left[box], high[item], low[item]) * size)


def final_kernel(pieces, out):
    out[...] = (pieces[0] + pieces[1]) + (pieces[2] + pieces[3])


def node_buffers(count):
    lead = () if count is None else (count,)
    return (
        pltpu.VMEM(lead + (2, BOXES, 1, NODES), jnp.float32),
        pltpu.VMEM(lead + (2, 2, 2, BOXES, 1, NODES), jnp.float32),
        pltpu.VMEM(lead + (2, CHEB, CHEB), jnp.float32),
        pltpu.VMEM(lead + (2, CHEB, CHEB), jnp.float32),
    )


TABLES = (
    pltpu.VMEM((BOXES, NODES, 128), jnp.float32),
    pltpu.VMEM((BOXES, NODES, 128), jnp.float32),
    pltpu.VMEM((2, CHEB, NODES), jnp.float32),
    pltpu.VMEM((2, CHEB, NODES), jnp.float32),
)
FIELD = (2, BOXES, RHS, NODES)
LEFT = pltpu.VMEM((BOXES, 4 * RHS, 2 * NODES), jnp.bfloat16)
STAGE = pltpu.VMEM((FOREIGN,) + FIELD, jnp.float32)
ANY = pl.BlockSpec(memory_space=pltpu.HBM)
WHOLE = pl.BlockSpec(memory_space=pltpu.VMEM)
PARAMS = pltpu.CompilerParams(vmem_limit_bytes=12 * 1024 * 1024)


SENT = pltpu.HBM((4,) + FIELD, jnp.float32)
KEPT = pltpu.VMEM(FIELD, jnp.float32)
SPREAD = pltpu.VMEM((2, CHEB, NODES), jnp.float32)
SMALL = pltpu.VMEM((2, CHEB, CHEB), jnp.float32)
PAIR = pltpu.VMEM((BOXES, 2 * NODES, NODES), jnp.bfloat16)
COLUMNS = pltpu.VMEM((BOXES, NODES, 128), jnp.float32)
MADE = pltpu.VMEM((ITEMS, 2 * NODES, NODES), jnp.bfloat16)


def far(x):
    return pltpu.with_memory_space_constraint(x, pltpu.HBM)


def cost(flops):
    return pl.CostEstimate(flops=flops, bytes_accessed=100_000, transcendentals=0)


def solution(mesh):
    groups = [group_members(mesh, bit) for bit in range(LEVELS)]

    def exchange(sent, level):
        return lax.all_to_all(
            sent, ("sx", "sy"), 0, 0, axis_index_groups=groups[level], tiled=True
        )

    def local(coeffs, source_nodes, target_nodes, interp_rows, interp_cols):
        current = coeffs.reshape(FIELD)
        nodes = (
            far(source_nodes.reshape(LEVELS, 2, BOXES, 1, NODES)),
            far(target_nodes.reshape(LEVELS, 2, 2, 2, BOXES, 1, NODES)),
            far(interp_rows),
            far(interp_cols),
        )
        packed, rows, cols = pl.pallas_call(
            pack_kernel,
            in_specs=[ANY] * 5,
            out_specs=[WHOLE] * 3,
            out_shape=[pltpu.VMEM((PACKED, NODES), jnp.float32), SMALL, SMALL],
            scratch_shapes=(KEPT,) + node_buffers(None)[:2] + (pltpu.SemaphoreType.DMA((5,)),),
            compiler_params=PARAMS,
            name="pack",
        )(far(current), *nodes)
        got = swapped(packed, "sy")
        sources1, targets1, rows1, cols1 = node_buffers(None)
        partial, row0, col0, a_near, b_near, *tables1 = pl.pallas_call(
            near_kernel,
            in_specs=[WHOLE] * 3 + [ANY] * 4,
            out_specs=[WHOLE] * 10,
            out_shape=[KEPT, SPREAD, SPREAD, COLUMNS, COLUMNS]
            + [COLUMNS, COLUMNS, SPREAD, SPREAD, targets1],
            scratch_shapes=(PAIR, PAIR, sources1, rows1, cols1, pltpu.SemaphoreType.DMA((4,))),
            compiler_params=PARAMS,
            cost_estimate=cost(20_000_000),
            name="near",
        )(packed, rows, cols, *nodes)
        sent, a_got, b_got = pl.pallas_call(
            partner_kernel,
            in_specs=[WHOLE] * 4,
            out_specs=[WHOLE] * 3,
            out_shape=[KEPT, COLUMNS, COLUMNS],
            scratch_shapes=(PAIR, PAIR),
            compiler_params=PARAMS,
            name="partner",
        )(got, row0, col0, partial)
        own, high, low = pl.pallas_call(
            second_kernel,
            in_specs=[WHOLE] * 13,
            out_specs=[WHOLE] * 3,
            out_shape=[KEPT, MADE, MADE],
            scratch_shapes=(PAIR, PAIR),
            compiler_params=PARAMS,
            cost_estimate=cost(60_000_000),
            name="second",
        )(packed, got, row0, col0, a_near, b_near, a_got, b_got, *tables1)
        pieces = swapped(sent, "sx")
        sent, current = pl.pallas_call(
            middle_kernel,
            in_specs=[WHOLE] * 4,
            out_specs=[ANY, WHOLE],
            out_shape=[SENT, KEPT],
            scratch_shapes=(LEFT, STAGE, pltpu.SemaphoreType.DMA((FOREIGN,))),
            compiler_params=PARAMS,
            name="middle",
        )(pieces, own, high, low)
        made = pl.pallas_call(
            between_kernel,
            in_specs=[WHOLE] + [ANY] * 4,
            out_specs=[WHOLE] * 5,
            out_shape=[
                KEPT,
                pltpu.VMEM((4 * BOXES, 2 * NODES, NODES), jnp.bfloat16),
                pltpu.VMEM((4 * BOXES, 2 * NODES, NODES), jnp.float8_e4m3fn),
                pltpu.VMEM((2, 128), jnp.float32),
                pltpu.VMEM((2, 128), jnp.float32),
            ],
            scratch_shapes=node_buffers(2)
            + TABLES
            + (PAIR, PAIR, LEFT, SMALL, SMALL, pltpu.SemaphoreType.DMA((4,))),
            compiler_params=PARAMS,
            cost_estimate=cost(60_000_000),
            name="between",
        )(current, *nodes)
        pieces = exchange(sent, 1)
        sent = pl.pallas_call(
            late_kernel,
            in_specs=[WHOLE] * 6,
            out_specs=WHOLE,
            out_shape=pltpu.VMEM((4,) + FIELD, jnp.float32),
            scratch_shapes=(LEFT,),
            compiler_params=PARAMS,
            name="late",
        )(pieces, *made)
        field = pl.pallas_call(
            final_kernel,
            in_specs=[WHOLE],
            out_specs=WHOLE,
            out_shape=jax.ShapeDtypeStruct(FIELD, jnp.float32),
            compiler_params=PARAMS,
            name="final",
        )(exchange(sent, 2))
        return field.reshape(2, BOXES, 1, RHS, NODES)

    in_specs = (
        P(None, "sx", "sy", None, None),
        P(None, None, "sx", "sy", None),
        P(None, None, None, None, "sx", "sy", None),
        P(),
        P(),
    )
    out_specs = P(None, "sx", "sy", None, None)
    return jax.shard_map(local, mesh=mesh, in_specs=in_specs, out_specs=out_specs, check_vma=False)
```
